16 devices in a mesh: rep: 2 (over y, z), dp: 8 (over x, core).
Axes of the slice: x: 4, y: 2, z: 1, core: 2. Of those that a mesh axis runs over, the one named last changes fastest.
The devices are a block of a 4x4x8 slice.
Arguments:
- x: bfloat16 [16, 2048, 1024], P(('rep', 'dp')), parts along dimension 0
- dy: bfloat16 [16, 2048, 1024], P(('rep', 'dp')), parts along dimension 0
- w_gate: bfloat16 [2, 1024, 4096], replicated
- w_up: bfloat16 [2, 1024, 4096], replicated
- w_down: bfloat16 [2, 4096, 1024], replicated
- m_w_gate: float32 [2, 1024, 4096], P(None, 'dp')
- m_w_up: float32 [2, 1024, 4096], P(None, 'dp')
- m_w_down: float32 [2, 4096, 1024], P(None, 'dp')
- v_w_gate: float32 [2, 1024, 4096], P(None, 'dp')
- v_w_up: float32 [2, 1024, 4096], P(None, 'dp')
- v_w_down: float32 [2, 4096, 1024], P(None, 'dp')
Outputs:
- output 1: bfloat16 [4, 1024, 4096], P('rep'), parts along dimension 0
- output 2: bfloat16 [4, 1024, 4096], P('rep'), parts along dimension 0
- output 3: bfloat16 [4, 4096, 1024], P('rep'), parts along dimension 0
- output 4: float32 [4, 1024, 4096], P('rep', 'dp'), parts along dimension 0
- output 5: float32 [4, 1024, 4096], P('rep', 'dp'), parts along dimension 0
- output 6: float32 [4, 4096, 1024], P('rep', 'dp'), parts along dimension 0
- output 7: float32 [4, 1024, 4096], P('rep', 'dp'), parts along dimension 0
- output 8: float32 [4, 1024, 4096], P('rep', 'dp'), parts along dimension 0
- output 9: float32 [4, 4096, 1024], P('rep', 'dp'), parts along dimension 0
There are 2 independent parts. The reference program is written for one: setup_inputs(seed, part) draws one part's arguments, and reference() takes and returns one part's arrays. A program takes and returns all parts, laid end to end along the dimension named above; an argument that names none is the same for every part.
All inputs are finite; a program needn't handle non-finite values.
Results may differ from the reference program's by a relative error of at most 0.0221.
Values are sent between devices in bfloat16 or wider.
A program may use at most 768 MiB of HBM per device.

```python
import jax
import jax.numpy as jnp
from jax import lax

SEQUENCES = 8
TOKENS = 2048
D = 1024
FF = 4096
LAYERS = 2
NAMES = ("w_gate", "w_up", "w_down")
SHAPES = {"w_gate": (LAYERS, D, FF), "w_up": (LAYERS, D, FF), "w_down": (LAYERS, FF, D)}


def bump(key, n, height):
    away = (jnp.arange(n, dtype=jnp.int32) - jax.random.randint(key, (), 0, n, jnp.int32)) % n
    return jnp.where(away < n // 8, height, 1.0)


def together(key, own, strength):
    shared = jax.random.normal(key, own.shape[1:], jnp.float32)
    return (own + strength * shared) * lax.rsqrt(1 + strength * strength)


def setup_inputs(seed: int = 0, part: int = 0) -> dict:
    kx, kdy, ka, kb, kz, kf, kh, kl, *keys = jax.random.split(jax.random.key(seed), 8 + 3 * len(NAMES))
    kx, kdy, ka, kb = (jax.random.fold_in(k, part) for k in (kx, kdy, ka, kb))
    kw, km, kv = (keys[i::3] for i in range(3))
    shape = (SEQUENCES, TOKENS, D)
    much_x, much_dy = jax.random.uniform(kz, (2,), jnp.float32, 0.0, 1.0)
    loud = 2.0 ** jax.random.uniform(jax.random.fold_in(kz, 1), (), jnp.float32, -1.0, 2.0)
    layers = 2.0 ** jax.random.uniform(kl, (LAYERS, 1, 1), jnp.float32, -1.0, 1.0)
    x = together(ka, jax.random.normal(kx, shape, jnp.float32), much_x) * bump(kf, D, 4.0)
    dy = together(kb, jax.random.normal(kdy, shape, jnp.float32), much_dy)
    drawn = {"x": x.astype(jnp.bfloat16), "dy": (loud * dy * (SEQUENCES * TOKENS) ** -0.5).astype(jnp.bfloat16)}
    for key, name in zip(kw, NAMES, strict=True):
        w = jax.random.normal(key, SHAPES[name], jnp.float32) * SHAPES[name][1] ** -0.5
        drawn[name] = (w * {"w_gate": 1.0, "w_up": bump(kh, FF, 4.0), "w_down": layers}[name]).astype(jnp.bfloat16)
    for key, name in zip(km, NAMES, strict=True):
        drawn[f"m_{name}"] = 0.1 * jax.random.normal(key, SHAPES[name], jnp.float32)
    for key, name in zip(kv, NAMES, strict=True):
        drawn[f"v_{name}"] = jax.random.uniform(key, SHAPES[name], jnp.float32, 0.005, 0.015)
    return drawn


def matmul(a, w):
    return jnp.dot(a, w, preferred_element_type=jnp.float32).astype(jnp.bfloat16)


def normed(h):
    wide = h.astype(jnp.float32)
    scale = lax.rsqrt(jnp.mean(wide**2, -1, keepdims=True) + 1e-6)
    return (wide * scale).astype(jnp.bfloat16)


def layer(h, w):
    a = normed(h)
    gate = jnp.dot(a, w["w_gate"], preferred_element_type=jnp.float32)
    up = jnp.dot(a, w["w_up"], preferred_element_type=jnp.float32)
    return h + matmul((jax.nn.silu(gate) * up).astype(jnp.bfloat16), w["w_down"])


def adamw(w, m, v, g):
    m = 0.9 * m + 0.1 * g
    v = 0.95 * v + 0.05 * g * g
    step = m * lax.rsqrt(v + 1e-8) + 0.1 * w
    return (w - 0.02 * step).astype(jnp.bfloat16), m, v


def stack(weights, h):
    return lax.scan(lambda h, w: (layer(h, w), None), h, weights)[0]


def reference(x, dy, w_gate, w_up, w_down, m_w_gate, m_w_up, m_w_down, v_w_gate, v_w_up, v_w_down):
    weights = dict(zip(NAMES, (w_gate, w_up, w_down), strict=True))

    def take(so_far, sequence):
        h, by_y = sequence
        _, back = jax.vjp(lambda w: stack(w, h), weights)
        return jax.tree.map(lambda total, term: total + term.astype(jnp.float32), so_far, back(by_y)[0]), None

    none_yet = {name: jnp.zeros(w.shape, jnp.float32) for name, w in weights.items()}
    by_weights, _ = lax.scan(take, none_yet, (x, dy))
    gradients = [by_weights[name].astype(jnp.bfloat16).astype(jnp.float32) for name in NAMES]
    new = [
        adamw(w.astype(jnp.float32), m, v, g)
        for w, m, v, g in zip((w_gate, w_up, w_down), (m_w_gate, m_w_up, m_w_down), (v_w_gate, v_w_up, v_w_down), gradients, strict=True)
    ]
    return tuple(one[which] for which in range(3) for one in new)
```

```python
import functools
import types

import jax
import jax.numpy as jnp
from jax import lax
from jax.experimental import pallas as pl
from jax.experimental.pallas import tpu as pltpu
from jax.sharding import PartitionSpec as P

MESH = pl.DeviceIdType.MESH
F32, BF = jnp.float32, jnp.bfloat16
LANES = 128


def dot(a, b, ca, cb):
    return lax.dot_general(a, b, (((ca,), (cb,)), ((), ())), preferred_element_type=F32)


def normed(h):
    wide = h.astype(F32)
    return (wide * lax.rsqrt(jnp.mean(wide * wide, -1, keepdims=True) + 1e-6)).astype(BF)


def new_weight(m, v, w, g):
    m = 0.9 * m + 0.1 * g
    v = 0.95 * v + 0.05 * g * g
    return w - 0.02 * (m * lax.rsqrt(v + 1e-8) + 0.1 * w)


def first_layer_kernel(steps, rows, x, wg, wu, wd, a0, h1, a1, act, acc):
    s = pl.program_id(0)
    tokens = x.shape[0]
    blocks = [pl.ds(r, rows) for r in range(0, tokens, rows)]

    @pl.when(s == 0)
    def _():
        for r in blocks:
            a0[r, :] = normed(x[r, :])
        acc[...] = jnp.zeros_like(acc)

    for r in blocks:
        g = dot(a0[r, :], wg[...], 1, 0)
        u = dot(a0[r, :], wu[...], 1, 0)
        act[r, :] = (g * (0.5 * jnp.tanh(0.5 * g) + 0.5) * u).astype(BF)
    for r in blocks:
        acc[r, :] += dot(act[r, :], wd[...], 1, 0)

    @pl.when(s == steps - 1)
    def _():
        for r in blocks:
            h = (x[r, :].astype(F32) + acc[r, :].astype(BF).astype(F32)).astype(BF)
            h1[r, :] = h
            a1[r, :] = normed(h)


def first_layer(x, w_gate, w_up, w_down):
    tokens, d = x.shape
    ff = w_gate.shape[2]
    tile = 4 * LANES
    steps = ff // tile
    whole = pl.BlockSpec((tokens, d), lambda s: (0, 0), pipeline_mode=pl.Buffered(1))
    return pl.pallas_call(
        functools.partial(first_layer_kernel, steps, 512),
        grid=(steps,),
        in_specs=[
            whole,
            pl.BlockSpec((None, d, tile), lambda s: (0, 0, s)),
            pl.BlockSpec((None, d, tile), lambda s: (0, 0, s)),
            pl.BlockSpec((None, tile, d), lambda s: (0, s, 0)),
        ],
        out_specs=[whole] * 3,
        out_shape=[jax.ShapeDtypeStruct((tokens, d), BF)] * 3,
        scratch_shapes=[pltpu.VMEM((tokens, tile), BF), pltpu.VMEM((tokens, d), F32)],
        compiler_params=pltpu.CompilerParams(vmem_limit_bytes=56 << 20),
        cost_estimate=pl.CostEstimate(flops=6 * tokens * d * ff, bytes_accessed=40 << 20, transcendentals=tokens * ff),
        name="first_layer",
    )(x, w_gate, w_up, w_down)


def step_kernel(z, *refs):
    (a1, dy, h1, a0, wg, wu, wd, mg, mu, md, vg, vu, vd, gown, wown, agw, a, dh, acc, act, dgs, dus, wbg, wbu, wbd), rest = refs[:25], refs[25:]
    families, (wsem, asem, adr, afs, afr, aps, apr) = rest[:36], rest[36:]
    names = ("u", "r0", "ra", "rb", "sa", "sb", "m", "v", "w", "gst", "wst", "q0", "q1s", "q1r", "q2s", "q2r", "cred", "qm")
    gu = types.SimpleNamespace(**dict(zip(names, families[:18], strict=True)), ns=z.ns_gu, total=2 * z.nt, first=z.nt, base=0)
    de = types.SimpleNamespace(**dict(zip(names, families[18:], strict=True)), ns=z.ns_d, total=2 * z.nq, first=z.nq, base=z.nt)
    gu.qo, gu.qg = gu.qm.at[3:11], gu.qm.at[11:13]
    de.qo, de.qg = de.qm.at[3:11], de.qm.at[11:13]

    me = lax.axis_index("dp")
    c, k = me // 2, me % 2
    cp, cm, co = (c + 1) % z.chips, (c + z.chips - 1) % z.chips, (c + 2) % z.chips
    partner, plus, minus = 2 * c + 1 - k, 2 * cp + k, 2 * cm + k
    im, ip, io = 2 * cm + k, 2 * cp + k, 2 * co + k
    half = z.rows // 2
    lo, hi = pl.ds(0, half), pl.ds(half, half)
    to = (plus, minus)

    def rcopy(src, dst, ssem, rsem, dev):
        return pltpu.make_async_remote_copy(src_ref=src, dst_ref=dst, send_sem=ssem, recv_sem=rsem, device_id={"dp": dev}, device_id_type=MESH)

    barrier = pltpu.get_barrier_semaphore()
    for dev in (partner, plus, minus):
        pl.semaphore_signal(barrier, inc=1, device_id={"dp": dev}, device_id_type=MESH)

    def where(t):
        s = t % z.nt
        return 1 - t // z.nt, s // z.nh, s % z.nh

    def run_at(q, h, j):
        return pl.ds(pl.multiple_of(z.fd * (z.j * h + j) + LANES * q, LANES), LANES)

    def fetch(t, slot):
        l, q, h = where(t)
        for j in range(z.j):
            f, b = run_at(q, h, j), pl.ds(LANES * j, LANES)
            pltpu.make_async_copy(wg.at[l, :, f], wbg.at[slot, :, b], wsem.at[slot, 0]).start()
            pltpu.make_async_copy(wu.at[l, :, f], wbu.at[slot, :, b], wsem.at[slot, 1]).start()
            pltpu.make_async_copy(wd.at[l, f, :], wbd.at[slot, b, :], wsem.at[slot, 2]).start()

    def fetched(slot):
        pltpu.make_async_copy(wg.at[0, :, pl.ds(0, z.tile)], wbg.at[slot], wsem.at[slot, 0]).wait()
        pltpu.make_async_copy(wu.at[0, :, pl.ds(0, z.tile)], wbu.at[slot], wsem.at[slot, 1]).wait()
        pltpu.make_async_copy(wd.at[0, pl.ds(0, z.tile), :], wbd.at[slot], wsem.at[slot, 2]).wait()

    def part(f, slot, x, r):
        return f.u[slot, x, k, r, :].astype(F32) + f.r0[slot, x, r, :].astype(F32)

    def pair_copy(f, slot):
        return rcopy(f.u.at[slot, :, 1 - k], f.r0.at[slot], f.q0.at[slot, 0], f.q0.at[slot, 1], partner)

    def far_copy(f, slot, d):
        return rcopy(f.sa.at[d], f.ra.at[slot, d], f.q1s.at[d], f.q1r.at[slot, d], to[d])

    def near_copy(f, slot, d):
        return rcopy(f.sb.at[d], f.rb.at[slot, d], f.q2s.at[d], f.q2r.at[slot, d], to[d])

    def s0(f, v):
        slot = v % f.ns

        @pl.when(v >= f.ns)
        def _():
            pl.semaphore_wait(f.cred.at[0], 1)

        pair_copy(f, slot).start()

    def s1(f, v):
        slot = v % f.ns
        pair_copy(f, slot).wait_recv()

        @pl.when(v >= f.ns)
        def _():
            pl.semaphore_wait(f.cred.at[1], 1)
            pl.semaphore_wait(f.cred.at[2], 1)

        f.sa[0, lo, :] = part(f, slot, co, lo).astype(BF)
        f.sa[0, hi, :] = part(f, slot, cp, hi).astype(BF)
        f.sa[1, lo, :] = part(f, slot, cm, lo).astype(BF)
        f.sa[1, hi, :] = part(f, slot, co, hi).astype(BF)
        for d in range(2):
            far_copy(f, slot, d).start()

    def s2(f, v):
        slot = v % f.ns
        for d in range(2):
            far_copy(f, slot, d).wait_recv()
            far_copy(f, slot, d).wait_send()
        f.sb[0] = (part(f, slot, cp, lo) + f.ra[slot, 0, lo, :].astype(F32)).astype(BF)
        f.sb[1] = (part(f, slot, cm, hi) + f.ra[slot, 1, hi, :].astype(F32)).astype(BF)
        for d in range(2):
            near_copy(f, slot, d).start()
        f.load(v)

    def agw_out(f, v, ws, x):
        return rcopy(f.wst.at[ws], agw.at[f.base + v, me], f.qo.at[4 * ws + x], (adr.at[f.base + v, 0], adr.at[f.base + v, 1], apr.at[f.base + v, 0])[x], (plus, minus, partner)[x])

    def own_out(f, v, ws):
        return pltpu.make_async_copy(f.wst.at[ws], agw.at[f.base + v, me], f.qo.at[4 * ws + 3])

    def last_out(f, v, ws):
        return pltpu.make_async_copy(f.wst.at[ws], wown.at[f.base + v - f.first], f.qo.at[4 * ws + 3])

    def grad_out(f, v, ws):
        l = v // f.first
        return pltpu.make_async_copy(f.gst.at[ws], gown.at[l * (z.nt + z.nq) + f.base + v % f.first], f.qg.at[ws])

    def sent(f, v, ws):
        grad_out(f, v, ws).wait()

        @pl.when(v < f.first)
        def _():
            for x in range(3):
                agw_out(f, v, ws, x).wait_send()
            own_out(f, v, ws).wait()

        @pl.when(v >= f.first)
        def _():
            last_out(f, v, ws).wait()

    def s3(f, v):
        slot, ws = v % f.ns, v % 2

        @pl.when(v >= 2)
        def _():
            sent(f, v - 2, ws)

        for d in range(2):
            near_copy(f, slot, d).wait_recv()
            near_copy(f, slot, d).wait_send()
        pair_copy(f, slot).wait_send()
        f.loaded()
        for r, x in ((lo, 0), (hi, 1)):
            g = part(f, slot, c, r) + f.ra[slot, 1 - x, r, :].astype(F32) + f.rb[slot, x].astype(F32)
            g = g.astype(BF)
            f.gst[ws, r, :] = g
            f.wst[ws, r, :] = new_weight(f.m[r, :], f.v[r, :], f.w[r, :].astype(F32), g.astype(F32)).astype(BF)

        @pl.when(v + f.ns < f.total)
        def _():
            for x, dev in enumerate((partner, plus, minus)):
                pl.semaphore_signal(f.cred.at[x], inc=1, device_id={"dp": dev}, device_id_type=MESH)

        grad_out(f, v, ws).start()

        @pl.when(v < f.first)
        def _():
            for x in range(3):
                agw_out(f, v, ws, x).start()
            own_out(f, v, ws).start()

        @pl.when(v >= f.first)
        def _():
            last_out(f, v, ws).start()

    def near_in(u, d):
        return rcopy(agw.at[u, (im, ip)[d]], agw.at[u, (im, ip)[d]], aps.at[u, 0], adr.at[u, d], to[d])

    def onward(u, d):
        x, r = ((im, lo), (ip, hi))[d]
        return rcopy(agw.at[u, x, r], agw.at[u, x, r], afs.at[u, d], afr.at[u, d], to[d])

    def far_in(u, d):
        r = (lo, hi)[d]
        return rcopy(agw.at[u, io, r], agw.at[u, io, r], afs.at[u, d], afr.at[u, d], to[d])

    def across(u, x):
        b = (im, ip, io)[x]
        return rcopy(agw.at[u, b], agw.at[u, b], aps.at[u, x], apr.at[u, x + 1], partner)

    def across_in(u, x):
        b = 2 * (c, cm, cp, co)[x] + 1 - k
        return rcopy(agw.at[u, b], agw.at[u, b], aps.at[u, 0], apr.at[u, x], partner)

    def s5(f, v):
        for d in range(2):
            near_in(f.base + v, d).wait_recv()
            onward(f.base + v, d).start()
            across(f.base + v, d).start()

    def s6(f, v):
        for d in range(2):
            far_in(f.base + v, d).wait_recv()
        across(f.base + v, 2).start()

    def load_gu(v):
        l, q, h = where(v)
        for j in range(z.j):
            fr = run_at(q, h, j)
            for x, (m, vv, w) in enumerate(((mg, vg, wg), (mu, vu, wu))):
                b = pl.ds(z.tile * x + LANES * j, LANES)
                pltpu.make_async_copy(m.at[l, :, fr], gu.m.at[:, b], gu.qm.at[0]).start()
                pltpu.make_async_copy(vv.at[l, :, fr], gu.v.at[:, b], gu.qm.at[1]).start()
                pltpu.make_async_copy(w.at[l, pl.ds(me * z.rows, z.rows), fr], gu.w.at[:, b], gu.qm.at[2]).start()

    def loaded_gu():
        width = pl.ds(0, 2 * z.tile)
        pltpu.make_async_copy(mg.at[0, :, width], gu.m, gu.qm.at[0]).wait()
        pltpu.make_async_copy(vg.at[0, :, width], gu.v, gu.qm.at[1]).wait()
        pltpu.make_async_copy(wg.at[0, pl.ds(0, z.rows), width], gu.w, gu.qm.at[2]).wait()

    def d_copies(v):
        l, q = 1 - v // z.nq, v % z.nq
        r = pl.ds(pl.multiple_of(q * z.rows, z.rows), z.rows)
        return (
            pltpu.make_async_copy(md.at[l, r, :], de.m, de.qm.at[0]),
            pltpu.make_async_copy(vd.at[l, r, :], de.v, de.qm.at[1]),
            pltpu.make_async_copy(wd.at[l, pl.ds(pl.multiple_of(me * z.fd + q * z.rows, z.rows), z.rows), :], de.w, de.qm.at[2]),
        )

    def load_d(v):
        for copy in d_copies(v):
            copy.start()

    def loaded_d():
        for copy in d_copies(0):
            copy.wait()

    gu.load, gu.loaded, de.load, de.loaded = load_gu, loaded_gu, load_d, loaded_d

    def run(stage, f, v, ok, count):
        @pl.when(jnp.logical_and(ok, jnp.logical_and(v >= 0, v < count)))
        def _():
            stage(f, v)

    pltpu.make_async_copy(a1, a, asem.at[0]).start()
    pltpu.make_async_copy(dy, dh, asem.at[1]).start()
    fetch(0, 0)
    acc[...] = jnp.zeros_like(acc)
    pltpu.make_async_copy(dy, dh, asem.at[1]).wait()
    pl.semaphore_wait(barrier, 3)

    blocks = [pl.ds(r, z.block) for r in range(0, z.tokens, z.block)]
    end = 2 * z.nt

    @pl.loop(0, end + 3)
    def _(t):
        slot, odd = t % 2, t % 2 == 1
        even = jnp.logical_not(odd)
        working = t < end

        @pl.when(working)
        def _():
            fetched(slot)

            @pl.when(t + 1 < end)
            def _():
                fetch(t + 1, 1 - slot)

        run(s3, gu, t - 2, True, gu.total)
        run(s1, de, (t - 2) // 2, even, de.total)

        @pl.when(working)
        def _():
            @pl.when(t % z.nt == 0)
            def _():
                pltpu.make_async_copy(a1, a, asem.at[0]).wait()

            for r in blocks:
                da = dot(dh[r, :], wbd[slot], 1, 1).astype(BF).astype(F32)
                g = dot(a[r, :], wbg[slot], 1, 0)
                u = dot(a[r, :], wbu[slot], 1, 0)
                s = 0.5 * jnp.tanh(0.5 * g) + 0.5
                gs = g * s
                act[r, :] = (gs * u).astype(BF)
                dgs[r, :] = (da * (u * (s + gs * (1.0 - s)))).astype(BF)
                dus[r, :] = (da * gs).astype(BF)

        run(s2, gu, t - 1, True, gu.total)
        run(s3, de, (t - 3) // 2, odd, de.total)
        run(s5, de, (t - 4) // 2, even, de.first)
        run(s6, de, (t - 5) // 2, odd, de.first)

        @pl.when(working)
        def _():
            us = t % gu.ns
            shape = (z.chips, 2, z.rows, z.tile)
            gu.u[us, :, :, :, : z.tile] = dot(a[...], dgs[...], 0, 0).astype(BF).reshape(shape)
            gu.u[us, :, :, :, z.tile :] = dot(a[...], dus[...], 0, 0).astype(BF).reshape(shape)

            @pl.when(t == z.nt - 1)
            def _():
                pltpu.make_async_copy(h1, a, asem.at[0]).start()

        run(s0, gu, t, True, gu.total)
        run(s2, de, (t - 2) // 2, even, de.total)
        run(s5, gu, t - 3, True, gu.first)
        run(s6, gu, t - 4, True, gu.first)

        @pl.when(working)
        def _():
            gd = dot(act[...], dh[...], 0, 0).astype(BF).reshape(z.j // 2, 2, z.rows, z.d)
            de.u[(t // 2) % de.ns, pl.ds((t % 2) * (z.j // 2), z.j // 2)] = gd

        run(s1, gu, t, True, gu.total)
        run(s0, de, (t - 1) // 2, odd, de.total)

        @pl.when(t < z.nt)
        def _():
            for r in blocks:
                acc[r, :] += dot(dgs[r, :], wbg[slot], 1, 1) + dot(dus[r, :], wbu[slot], 1, 1)

        @pl.when(t == z.nt - 1)
        def _():
            pltpu.make_async_copy(h1, a, asem.at[0]).wait()

            @pl.loop(0, z.tokens // z.block)
            def _(i):
                r = pl.ds(pl.multiple_of(i * z.block, z.block), z.block)
                h = a[r, :].astype(F32)
                da = acc[r, :].astype(BF).astype(F32)
                s = lax.rsqrt(jnp.mean(h * h, -1, keepdims=True) + 1e-6)
                along = jnp.mean(da * h, -1, keepdims=True)
                by_h = (s * da - h * (s * s * s * along)).astype(BF)
                dh[r, :] = (dh[r, :].astype(F32) + by_h.astype(F32)).astype(BF)

            pltpu.make_async_copy(a0, a, asem.at[0]).start()

    for f in (gu, de):
        for v in (f.total - 2, f.total - 1):
            sent(f, v, v % 2)

    @pl.loop(0, z.nt + z.nq)
    def _(u):
        for d in range(2):
            onward(u, d).wait_send()
        for x in range(3):
            across(u, x).wait_send()
        for x in range(4):
            across_in(u, x).wait_recv()


def backward(n, a1, dy, h1, a0, weights, m, v):
    tokens, d = a1.shape
    ff = weights[0].shape[2]
    z = types.SimpleNamespace(tokens=tokens, d=d, ff=ff, chips=n // 2, rows=d // n, fd=ff // n, tile=d // 2, block=512, ns_gu=3, ns_d=2)
    z.j = z.tile // LANES
    z.nt = ff // z.tile
    z.nq = z.fd // LANES
    z.nh = n // z.j
    assert z.chips == 4 and z.rows == LANES and z.nh == 2
    units = z.nt + z.nq
    half = z.rows // 2

    def family(ns):
        dma, vm = pltpu.SemaphoreType.DMA, pltpu.VMEM
        return [
            vm((ns, z.chips, 2, z.rows, d), BF),
            vm((ns, z.chips, z.rows, d), BF),
            vm((ns, 2, z.rows, d), BF),
            vm((ns, 2, half, d), BF),
            vm((2, z.rows, d), BF),
            vm((2, half, d), BF),
            vm((z.rows, d), F32),
            vm((z.rows, d), F32),
            vm((z.rows, d), BF),
            vm((2, z.rows, d), BF),
            vm((2, z.rows, d), BF),
            dma((ns, 2)),
            dma((2,)),
            dma((ns, 2)),
            dma((2,)),
            dma((ns, 2)),
            pltpu.SemaphoreType.REGULAR((3,)),
            dma((13,)),
        ]

    dma, vm = pltpu.SemaphoreType.DMA, pltpu.VMEM
    return pl.pallas_call(
        functools.partial(step_kernel, z),
        in_specs=[pl.BlockSpec(memory_space=pl.ANY)] * 13,
        out_specs=[pl.BlockSpec(memory_space=pl.ANY)] * 3,
        out_shape=[
            jax.ShapeDtypeStruct((2 * units, z.rows, d), BF),
            jax.ShapeDtypeStruct((units, z.rows, d), BF),
            jax.ShapeDtypeStruct((units, n, z.rows, d), BF),
        ],
        scratch_shapes=[
            vm((tokens, d), BF),
            vm((tokens, d), BF),
            vm((tokens, d), F32),
            vm((tokens, z.tile), BF),
            vm((tokens, z.tile), BF),
            vm((tokens, z.tile), BF),
            vm((2, d, z.tile), BF),
            vm((2, d, z.tile), BF),
            vm((2, z.tile, d), BF),
            *family(z.ns_gu),
            *family(z.ns_d),
            dma((2, 3)),
            dma((2,)),
            dma((units, 2)),
            dma((units, 2)),
            dma((units, 2)),
            dma((units, 3)),
            dma((units, 4)),
        ],
        compiler_params=pltpu.CompilerParams(collective_id=0, has_side_effects=True, vmem_limit_bytes=67043328),
        cost_estimate=pl.CostEstimate(flops=28 * tokens * d * ff, bytes_accessed=200 << 20, transcendentals=2 * tokens * ff),
        name="backward",
    )(a1, dy, h1, a0, *weights, *m, *v)


def place_kernel(z, layer, sources, count, *refs):
    srcs, (og, ou, od) = refs[:count], refs[count + 3 : count + 6]
    buf, gate, up, isem, osem = refs[count + 6 :]
    me = lax.axis_index("dp")
    c, k = me // 2, me % 2

    def source(x):
        at, other, part = sources[x]
        b = 2 * ((c + at) % z.chips) + (1 - k if other else k)
        return b, part, srcs[x].shape[1]

    def load(x):
        return pltpu.make_async_copy(srcs[x], buf.at[x % 2, :, pl.ds(0, srcs[x].shape[1])], isem.at[x % 2])

    def stores(x):
        b, part, rows = source(x)
        r, s = pl.ds(part * rows, rows), pl.ds(0, rows)
        return (
            pltpu.make_async_copy(gate.at[x % 2, s], og.at[layer, b, r], osem.at[x % 2, 0]),
            pltpu.make_async_copy(up.at[x % 2, s], ou.at[layer, b, r], osem.at[x % 2, 1]),
            pltpu.make_async_copy(buf.at[x % 2, pl.ds(z.nt, z.nq), s], od.at[layer, b, :, r], osem.at[x % 2, 2]),
        )

    load(0).start()
    for x in range(count):
        load(x).wait()
        if x >= 1:
            for copy in stores(x - 1):
                copy.wait()
        if x + 1 < count:
            load(x + 1).start()
        rows = srcs[x].shape[1]
        for t in range(z.nt):
            q, h = t // z.nh, t % z.nh
            for j in range(z.j):
                col = z.fd * (z.j * h + j) + LANES * q
                gate[x % 2, :rows, col : col + LANES] = buf[x % 2, t, :rows, LANES * j : LANES * (j + 1)]
                up[x % 2, :rows, col : col + LANES] = buf[x % 2, t, :rows, z.tile + LANES * j : z.tile + LANES * (j + 1)]
        for copy in stores(x):
            copy.start()
    for copy in stores(count - 1):
        copy.wait()


def place(z, layer, sources, arrays, outs):
    count = len(arrays)
    size = sum(a.size for a in arrays) * 4
    return pl.pallas_call(
        functools.partial(place_kernel, z, layer, sources, count),
        in_specs=[pl.BlockSpec(memory_space=pl.ANY)] * (count + 3),
        out_specs=[pl.BlockSpec(memory_space=pl.ANY)] * 3,
        out_shape=[jax.ShapeDtypeStruct(o.shape, o.dtype) for o in outs],
        input_output_aliases={count + i: i for i in range(3)},
        scratch_shapes=[
            pltpu.VMEM((2, z.nt + z.nq, z.rows, z.d), BF),
            pltpu.VMEM((2, z.rows, z.ff), BF),
            pltpu.VMEM((2, z.rows, z.ff), BF),
            pltpu.SemaphoreType.DMA((2,)),
            pltpu.SemaphoreType.DMA((2, 3)),
        ],
        compiler_params=pltpu.CompilerParams(vmem_limit_bytes=24 << 20),
        cost_estimate=pl.CostEstimate(flops=size * 100, bytes_accessed=size, transcendentals=0),
        name="place",
    )(*arrays, *outs)


def spread_kernel(z, src, og, ou, od):
    for t in range(z.nt):
        q, h = t // z.nh, t % z.nh
        for j in range(z.j):
            col = z.fd * (z.j * h + j) + LANES * q
            og[:, col : col + LANES] = src[t, :, LANES * j : LANES * (j + 1)]
            ou[:, col : col + LANES] = src[t, :, z.tile + LANES * j : z.tile + LANES * (j + 1)]
    od[...] = src[z.nt :]


def spread(z, layers, layer, agw):
    n = agw.shape[1]
    return pl.pallas_call(
        functools.partial(spread_kernel, z),
        grid=(n,),
        in_specs=[pl.BlockSpec((z.nt + z.nq, None, z.rows, z.d), lambda b: (0, b, 0, 0))],
        out_specs=[
            pl.BlockSpec((None, None, z.rows, z.ff), lambda b: (layer, b, 0, 0)),
            pl.BlockSpec((None, None, z.rows, z.ff), lambda b: (layer, b, 0, 0)),
            pl.BlockSpec((None, None, z.nq, z.rows, z.d), lambda b: (layer, b, 0, 0, 0)),
        ],
        out_shape=[
            jax.ShapeDtypeStruct((layers, n, z.rows, z.ff), BF),
            jax.ShapeDtypeStruct((layers, n, z.rows, z.ff), BF),
            jax.ShapeDtypeStruct((layers, n, z.nq, z.rows, z.d), BF),
        ],
        compiler_params=pltpu.CompilerParams(vmem_limit_bytes=24 << 20),
        cost_estimate=pl.CostEstimate(flops=agw.size * 400, bytes_accessed=agw.size * 4, transcendentals=0),
        name="spread",
    )(agw)


def moments(m, v, g):
    return 0.9 * m + 0.1 * g, 0.95 * v + 0.05 * g * g


def solution(mesh):
    n = mesh.shape["dp"]

    def device(x, dy, w_gate, w_up, w_down, *mv):
        m, v = mv[:3], mv[3:]
        x, dy = x[0], dy[0]
        layers, d, ff = w_gate.shape
        a0, h1, a1 = first_layer(x, w_gate, w_up, w_down)
        gown, wown, agw = backward(n, a1, dy, h1, a0, (w_gate, w_up, w_down), m, v)

        z = types.SimpleNamespace(d=d, ff=ff, chips=n // 2, rows=d // n, fd=ff // n, tile=d // 2)
        z.j, z.nt, z.nq = z.tile // LANES, ff // z.tile, z.fd // LANES
        z.nh = n // z.j
        units = z.nt + z.nq
        half = z.rows // 2

        def shift(a, by):
            return lax.ppermute(a, "dp", [(i, (i + 2 * by) % n) for i in range(n)])

        def swap(a):
            return lax.ppermute(a, "dp", [(i, i ^ 1) for i in range(n)])

        near = [shift(wown, 1), shift(wown, -1)]
        far = [shift(near[0][:, :half], 1), shift(near[1][:, half:], -1)]
        pair = swap(wown)
        outs = spread(z, layers, 1, agw)
        outs = place(z, 0, ((0, False, 0), (0, True, 0)), [wown, pair], outs)
        pair_near = [swap(a) for a in near]
        outs = place(z, 0, ((-1, False, 0), (1, False, 0), (-1, True, 0), (1, True, 0)), [*near, *pair_near], outs)
        pair_far = [swap(a) for a in far]
        outs = place(z, 0, ((2, False, 0), (2, False, 1), (2, True, 0), (2, True, 1)), [*far, *pair_far], outs)
        new = [o.reshape(w.shape) for o, w in zip(outs, (w_gate, w_up, w_down), strict=True)]

        g = gown.reshape(layers, units, z.rows, d)[::-1].astype(F32)
        runs = g[:, : z.nt].reshape(layers, z.nq, z.nh, z.rows, 2, z.j, LANES).transpose(4, 0, 3, 2, 5, 1, 6).reshape(2, layers, z.rows, ff)
        grads = (runs[0], runs[1], g[:, z.nt :].reshape(layers, z.fd, d))
        new_m, new_v = zip(*(moments(a, b, c) for a, b, c in zip(m, v, grads, strict=True)), strict=True)
        return (*new, *new_m, *new_v)

    sharded = P(None, "dp", None)
    return jax.shard_map(
        device,
        mesh=mesh,
        in_specs=(P(("rep", "dp")), P(("rep", "dp")), P(), P(), P(), *[sharded] * 6),
        out_specs=(*[P("rep")] * 3, *[P("rep", "dp", None)] * 6),
        check_vma=False,
    )
```

```python
import functools
import types

import jax
import jax.numpy as jnp
from jax import lax
from jax.experimental import pallas as pl
from jax.experimental.pallas import tpu as pltpu
from jax.sharding import PartitionSpec as P

MESH = pl.DeviceIdType.MESH
F32, BF = jnp.float32, jnp.bfloat16
LANES = 128


def dot(a, b, ca, cb):
    return lax.dot_general(a, b, (((ca,), (cb,)), ((), ())), preferred_element_type=F32)


def normed(h):
    wide = h.astype(F32)
    return (wide * lax.rsqrt(jnp.mean(wide * wide, -1, keepdims=True) + 1e-6)).astype(BF)


def new_weight(m, v, w, g):
    m = 0.9 * m + 0.1 * g
    v = 0.95 * v + 0.05 * g * g
    return w - 0.02 * (m * lax.rsqrt(v + 1e-8) + 0.1 * w)


def step_kernel(z, *refs):
    (xs, dy, wg, wu, wd, mg, mu, md, vg, vu, vd, gown, wlo, whi, agw, h1, a0, dgx, dux, a, dh, acc, act, dgs, dus, wbg, wbu, wbd), rest = refs[:28], refs[28:]
    families, (wsem, asem, xsem, ads, adr, afs, afr, aps, apr) = rest[:36], rest[36:]
    names = ("u", "r0", "ra", "rb", "sa", "sb", "m", "v", "w", "gst", "wst", "q0", "q1s", "q1r", "q2s", "q2r", "cred", "qm")
    gu = types.SimpleNamespace(**dict(zip(names, families[:18], strict=True)), ns=z.ns_gu, total=2 * z.nt, first=z.nt, base=0)
    de = types.SimpleNamespace(**dict(zip(names, families[18:], strict=True)), ns=z.ns_d, total=2 * z.nq, first=z.nq, base=z.nt)
    gu.qo, gu.qg = gu.qm.at[3:7], gu.qm.at[7:9]
    de.qo, de.qg = de.qm.at[3:7], de.qm.at[7:9]

    me = lax.axis_index("dp")
    c, k = me // 2, me % 2
    cp, cm, co = (c + 1) % z.chips, (c + z.chips - 1) % z.chips, (c + 2) % z.chips
    partner, plus, minus = 2 * c + 1 - k, 2 * cp + k, 2 * cm + k
    im, ip, io = 2 * cm + k, 2 * cp + k, 2 * co + k
    half = z.rows // 2
    lo, hi = pl.ds(0, half), pl.ds(half, half)
    to = (plus, minus)

    def rcopy(src, dst, ssem, rsem, dev):
        return pltpu.make_async_remote_copy(src_ref=src, dst_ref=dst, send_sem=ssem, recv_sem=rsem, device_id={"dp": dev}, device_id_type=MESH)

    barrier = pltpu.get_barrier_semaphore()
    for dev in (partner, plus, minus):
        pl.semaphore_signal(barrier, inc=1, device_id={"dp": dev}, device_id_type=MESH)

    def where(t):
        s = t % z.nt
        return 1 - t // z.nt, s // z.nh, s % z.nh

    def run_at(q, h, j):
        return pl.ds(pl.multiple_of(z.fd * (z.j * h + j) + LANES * q, LANES), LANES)

    def fetch(t, slot):
        l, q, h = where(t)
        for j in range(z.j):
            f, b = run_at(q, h, j), pl.ds(LANES * j, LANES)
            pltpu.make_async_copy(wg.at[l, :, f], wbg.at[slot, :, b], wsem.at[slot, 0]).start()
            pltpu.make_async_copy(wu.at[l, :, f], wbu.at[slot, :, b], wsem.at[slot, 1]).start()
            pltpu.make_async_copy(wd.at[l, f, :], wbd.at[slot, b, :], wsem.at[slot, 2]).start()

    def fetched(slot):
        pltpu.make_async_copy(wg.at[0, :, pl.ds(0, z.tile)], wbg.at[slot], wsem.at[slot, 0]).wait()
        pltpu.make_async_copy(wu.at[0, :, pl.ds(0, z.tile)], wbu.at[slot], wsem.at[slot, 1]).wait()
        pltpu.make_async_copy(wd.at[0, pl.ds(0, z.tile), :], wbd.at[slot], wsem.at[slot, 2]).wait()

    def part(f, slot, x, r):
        return f.u[slot, x, k, r, :].astype(F32) + f.r0[slot, x, r, :].astype(F32)

    def pair_copy(f, slot):
        return rcopy(f.u.at[slot, :, 1 - k], f.r0.at[slot], f.q0.at[slot, 0], f.q0.at[slot, 1], partner)

    def far_copy(f, slot, d):
        return rcopy(f.sa.at[d], f.ra.at[slot, d], f.q1s.at[d], f.q1r.at[slot, d], to[d])

    def near_copy(f, slot, d):
        return rcopy(f.sb.at[d], f.rb.at[slot, d], f.q2s.at[d], f.q2r.at[slot, d], to[d])

    def s0(f, v):
        slot = v % f.ns

        @pl.when(v >= f.ns)
        def _():
            pl.semaphore_wait(f.cred.at[0], 1)

        pair_copy(f, slot).start()

    def s1(f, v):
        slot = v % f.ns
        pair_copy(f, slot).wait_recv()

        @pl.when(v >= f.ns)
        def _():
            pl.semaphore_wait(f.cred.at[1], 1)
            pl.semaphore_wait(f.cred.at[2], 1)

        f.sa[0, lo, :] = part(f, slot, co, lo).astype(BF)
        f.sa[0, hi, :] = part(f, slot, cp, hi).astype(BF)
        f.sa[1, lo, :] = part(f, slot, cm, lo).astype(BF)
        f.sa[1, hi, :] = part(f, slot, co, hi).astype(BF)
        for d in range(2):
            far_copy(f, slot, d).start()

    def s2(f, v):
        slot = v % f.ns
        for d in range(2):
            far_copy(f, slot, d).wait_recv()
            far_copy(f, slot, d).wait_send()
        f.sb[0] = (part(f, slot, cp, lo) + f.ra[slot, 0, lo, :].astype(F32)).astype(BF)
        f.sb[1] = (part(f, slot, cm, hi) + f.ra[slot, 1, hi, :].astype(F32)).astype(BF)
        for d in range(2):
            near_copy(f, slot, d).start()
        f.load(v)

    def own_out(f, v, ws):
        return pltpu.make_async_copy(f.wst.at[ws], agw.at[f.base + v, me], f.qo.at[2 * ws])

    def last_out(f, v, ws, x):
        u = f.base + v - f.first
        return pltpu.make_async_copy(f.wst.at[ws, (lo, hi)[x]], (wlo, whi)[x].at[u], f.qo.at[2 * ws + x])

    def grad_out(f, v, ws):
        l = v // f.first
        return pltpu.make_async_copy(f.gst.at[ws], gown.at[l * (z.nt + z.nq) + f.base + v % f.first], f.qg.at[ws])

    def sent(f, v, ws):
        grad_out(f, v, ws).wait()

        @pl.when(v >= f.first)
        def _():
            for x in range(2):
                last_out(f, v, ws, x).wait()

    def s3(f, v):
        slot, ws = v % f.ns, v % 2

        @pl.when(v >= 2)
        def _():
            sent(f, v - 2, ws)

        for d in range(2):
            near_copy(f, slot, d).wait_recv()
            near_copy(f, slot, d).wait_send()
        pair_copy(f, slot).wait_send()
        f.loaded()
        for r, x in ((lo, 0), (hi, 1)):
            g = part(f, slot, c, r) + f.ra[slot, 1 - x, r, :].astype(F32) + f.rb[slot, x].astype(F32)
            g = g.astype(BF)
            f.gst[ws, r, :] = g
            f.wst[ws, r, :] = new_weight(f.m[r, :], f.v[r, :], f.w[r, :].astype(F32), g.astype(F32)).astype(BF)

        @pl.when(v + f.ns < f.total)
        def _():
            for x, dev in enumerate((partner, plus, minus)):
                pl.semaphore_signal(f.cred.at[x], inc=1, device_id={"dp": dev}, device_id_type=MESH)

        grad_out(f, v, ws).start()

        @pl.when(v < f.first)
        def _():
            own_out(f, v, ws).start()

        @pl.when(v >= f.first)
        def _():
            for x in range(2):
                last_out(f, v, ws, x).start()

    def own_to(u, x):
        return rcopy(agw.at[u, me], agw.at[u, me], ads.at[u, x], (adr.at[u, 0], adr.at[u, 1], apr.at[u, 0])[x], (plus, minus, partner)[x])

    def near_in(u, d):
        return rcopy(agw.at[u, (im, ip)[d]], agw.at[u, (im, ip)[d]], aps.at[u, 0], adr.at[u, d], to[d])

    def onward(u, d):
        x, r = ((im, lo), (ip, hi))[d]
        return rcopy(agw.at[u, x, r], agw.at[u, x, r], afs.at[u, d], afr.at[u, d], to[d])

    def far_in(u, d):
        r = (lo, hi)[d]
        return rcopy(agw.at[u, io, r], agw.at[u, io, r], afs.at[u, d], afr.at[u, d], to[d])

    def across(u, x):
        b = (im, ip, io)[x]
        return rcopy(agw.at[u, b], agw.at[u, b], aps.at[u, x], apr.at[u, x + 1], partner)

    def across_in(u, x):
        b = 2 * (c, cm, cp, co)[x] + 1 - k
        return rcopy(agw.at[u, b], agw.at[u, b], aps.at[u, 0], apr.at[u, x], partner)

    def held(f, v):
        @pl.when(v < f.first)
        def _():
            own_out(f, v, v % 2).wait()

    def s4(u):
        for x in range(3):
            own_to(u, x).start()

    def s5(u):
        for d in range(2):
            near_in(u, d).wait_recv()
            onward(u, d).start()
            across(u, d).start()

    def s6(u):
        for d in range(2):
            far_in(u, d).wait_recv()
        across(u, 2).start()

    def load_gu(v):
        l, q, h = where(v)
        for j in range(z.j):
            fr = run_at(q, h, j)
            for x, (m, vv, w) in enumerate(((mg, vg, wg), (mu, vu, wu))):
                b = pl.ds(z.tile * x + LANES * j, LANES)
                pltpu.make_async_copy(m.at[l, :, fr], gu.m.at[:, b], gu.qm.at[0]).start()
                pltpu.make_async_copy(vv.at[l, :, fr], gu.v.at[:, b], gu.qm.at[1]).start()
                pltpu.make_async_copy(w.at[l, pl.ds(me * z.rows, z.rows), fr], gu.w.at[:, b], gu.qm.at[2]).start()

    def loaded_gu():
        width = pl.ds(0, 2 * z.tile)
        pltpu.make_async_copy(mg.at[0, :, width], gu.m, gu.qm.at[0]).wait()
        pltpu.make_async_copy(vg.at[0, :, width], gu.v, gu.qm.at[1]).wait()
        pltpu.make_async_copy(wg.at[0, pl.ds(0, z.rows), width], gu.w, gu.qm.at[2]).wait()

    def d_copies(v):
        l, q = 1 - v // z.nq, v % z.nq
        r = pl.ds(pl.multiple_of(q * z.rows, z.rows), z.rows)
        return (
            pltpu.make_async_copy(md.at[l, r, :], de.m, de.qm.at[0]),
            pltpu.make_async_copy(vd.at[l, r, :], de.v, de.qm.at[1]),
            pltpu.make_async_copy(wd.at[l, pl.ds(pl.multiple_of(me * z.fd + q * z.rows, z.rows), z.rows), :], de.w, de.qm.at[2]),
        )

    def load_d(v):
        for copy in d_copies(v):
            copy.start()

    def loaded_d():
        for copy in d_copies(0):
            copy.wait()

    gu.load, gu.loaded, de.load, de.loaded = load_gu, loaded_gu, load_d, loaded_d

    def run(stage, f, made, least=0):
        if f is de:
            odd, made = made % 2 == 1, (made - 1) // 2
        gap = z.gap if f is gu else z.gap // 2
        v = jnp.where(made < f.first, made, made - gap)
        ok = jnp.logical_or(jnp.logical_and(made >= least, made < f.first), jnp.logical_and(made >= f.first + gap, made < f.total + gap))

        @pl.when(ok if f is gu else jnp.logical_and(ok, odd))
        def _():
            stage(f, v)

    def gather(stage, table, s):
        while table:
            once = dict(table)
            table = [pair for pair in table if once[pair[0]] != pair[1]]
            u, ok = 0, False
            for at, unit in once.items():
                u = jnp.where(s == at, unit, u)
                ok = jnp.logical_or(ok, s == at)

            @pl.when(ok)
            def _(u=u):
                stage(u)

    blocks = [pl.ds(r, z.block) for r in range(0, z.tokens, z.block)]
    per = z.chips * 2 * z.rows // z.block
    width = z.block // (2 * z.rows)

    def held_rows(b):
        return (b // per, pl.ds(b % per * width, width))

    def states(b):
        return gu.u[held_rows(b)].reshape(z.block, z.d)

    held_states = gu.u.at[: z.tokens * z.d // (z.chips * 2 * z.rows * z.d)]

    pltpu.make_async_copy(xs, held_states, xsem.at[0]).start()
    pltpu.make_async_copy(dy, dh, asem.at[1]).start()
    fetch(z.nt, 0)
    acc[...] = jnp.zeros_like(acc)
    pltpu.make_async_copy(xs, held_states, xsem.at[0]).wait()
    for b, r in enumerate(blocks):
        a[r, :] = normed(states(b))
    pltpu.make_async_copy(a, a0, xsem.at[1]).start()

    @pl.loop(0, z.nt)
    def _(t):
        slot = t % 2
        fetched(slot)
        fetch(jnp.where(t + 1 < z.nt, t + 1 + z.nt, 0), 1 - slot)
        for r in blocks:
            g = dot(a[r, :], wbg[slot], 1, 0)
            u = dot(a[r, :], wbu[slot], 1, 0)
            act[r, :] = (g * (0.5 * jnp.tanh(0.5 * g) + 0.5) * u).astype(BF)
        for r in blocks:
            acc[r, :] += dot(act[r, :], wbd[slot], 1, 0)

    pltpu.make_async_copy(a, a0, xsem.at[1]).wait()
    for b, r in enumerate(blocks):
        h = (states(b).astype(F32) + acc[r, :].astype(BF).astype(F32)).astype(BF)
        gu.u[held_rows(b)] = h.reshape(width, 2, z.rows, z.d)
        a[r, :] = normed(h)
    acc[...] = jnp.zeros_like(acc)
    pltpu.make_async_copy(held_states, h1, xsem.at[0]).start()
    pltpu.make_async_copy(dy, dh, asem.at[1]).wait()
    pl.semaphore_wait(barrier, 3)

    end = 2 * z.nt + z.gap

    def spill(t, slot):
        return (
            pltpu.make_async_copy(dgs.at[slot], dgx.at[t], xsem.at[2]),
            pltpu.make_async_copy(dus.at[slot], dux.at[t], xsem.at[3]),
        )

    def unspill(t, slot):
        return (
            pltpu.make_async_copy(dgx.at[t], dgs.at[slot], xsem.at[4 + slot]),
            pltpu.make_async_copy(dux.at[t], dus.at[slot], xsem.at[6 + slot]),
        )

    def add_da(t, slot):
        @pl.when(t < z.nt - 2)
        def _():
            for copy in unspill(t, slot):
                copy.wait()
            fetched(slot)

        for r in blocks:
            acc[r, :] += dot(dgs[slot, r, :], wbg[slot], 1, 1) + dot(dus[slot, r, :], wbu[slot], 1, 1)

        @pl.when(t >= 2)
        def _():
            fetch(t - 2, slot)
            for copy in unspill(t - 2, slot):
                copy.start()

    @pl.loop(0, end + 3)
    def _(s):
        second = s >= z.nt + z.gap
        t = jnp.where(second, s - z.gap, s)
        slot = t % 2
        working = jnp.logical_and(s < end, jnp.logical_or(second, s < z.nt))
        adding = jnp.logical_and(s >= z.nt, jnp.logical_not(second))

        @pl.when(working)
        def _():
            fetched(slot)

            @pl.when(t % z.nt < z.nt - 1)
            def _():
                fetch(t + 1, 1 - slot)

        @pl.when(working)
        def _():
            @pl.when(t == z.nt)
            def _():
                pltpu.make_async_copy(a0, a, asem.at[0]).wait()

            for r in blocks:
                da = dot(dh[r, :], wbd[slot], 1, 1).astype(BF).astype(F32)
                g = dot(a[r, :], wbg[slot], 1, 0)
                u = dot(a[r, :], wbu[slot], 1, 0)
                sig = 0.5 * jnp.tanh(0.5 * g) + 0.5
                gs = g * sig
                act[r, :] = (gs * u).astype(BF)
                dgs[slot, r, :] = (da * (u * (sig + gs * (1.0 - sig)))).astype(BF)
                dus[slot, r, :] = (da * gs).astype(BF)

            @pl.when(t < z.nt - 2)
            def _():
                for copy in spill(t, slot):
                    copy.start()

        run(s1, de, s - 1)

        @pl.when(jnp.logical_and(s >= 1, s <= z.early))
        def _():
            s2(gu, s - 1)

        @pl.when(jnp.logical_and(s >= 2, s <= z.early + 1))
        def _():
            held(gu, s - 2)

        run(held, de, s - 3)
        gather(s4, z.s4b, s)
        gather(s5, z.s5b, s)
        gather(s6, z.s6b, s)

        @pl.when(s == 0)
        def _():
            pltpu.make_async_copy(held_states, h1, xsem.at[0]).wait()

        @pl.when(adding)
        def _():
            tile = 2 * z.nt - 1 - s
            add_da(tile, tile % 2)

        @pl.when(working)
        def _():
            us = t % gu.ns
            shape = (z.chips, 2, z.rows, z.tile)
            gu.u[us, :, :, :, : z.tile] = dot(a[...], dgs[slot], 0, 0).astype(BF).reshape(shape)
            gu.u[us, :, :, :, z.tile :] = dot(a[...], dus[slot], 0, 0).astype(BF).reshape(shape)

            @pl.when(t == z.nt - 1)
            def _():
                for b in range(z.tokens // z.rows):
                    at = h1.at[b // (2 * z.chips), b // 2 % z.chips, b % 2]
                    pltpu.make_async_copy(at, a.at[pl.ds(z.rows * b, z.rows)], asem.at[0]).start()

            @pl.when(t < z.nt - 2)
            def _():
                for copy in spill(t, slot):
                    copy.wait()

        run(s0, gu, s)
        run(held, gu, s - 3, z.early)
        run(s3, gu, s - 2, z.early)

        @pl.when(working)
        def _():
            gd = dot(act[...], dh[...], 0, 0).astype(BF).reshape(z.j // 2, 2, z.rows, z.d)
            de.u[(t // 2) % de.ns, pl.ds((t % 2) * (z.j // 2), z.j // 2)] = gd

        run(s2, gu, s - 1, z.early)
        run(s1, gu, s)
        run(s0, de, s)
        run(s2, de, s - 1)
        run(s3, de, s - 2)

        @pl.when(jnp.logical_and(s >= 1, s <= z.early))
        def _():
            s3(gu, s - 1)

        @pl.when(s == z.nt + z.gap - 1)
        def _():
            fetch(z.nt, 0)
            pltpu.make_async_copy(a0, a, asem.at[0]).wait()

            @pl.loop(0, z.tokens // z.block)
            def _(i):
                r = pl.ds(pl.multiple_of(i * z.block, z.block), z.block)
                h = a[r, :].astype(F32)
                da = acc[r, :].astype(BF).astype(F32)
                scale = lax.rsqrt(jnp.mean(h * h, -1, keepdims=True) + 1e-6)
                along = jnp.mean(da * h, -1, keepdims=True)
                by_h = (scale * da - h * (scale * scale * scale * along)).astype(BF)
                dh[r, :] = (dh[r, :].astype(F32) + by_h.astype(F32)).astype(BF)

            pltpu.make_async_copy(a0, a, asem.at[0]).start()

    for f in (gu, de):
        for v in (f.total - 2, f.total - 1):
            sent(f, v, v % 2)

    @pl.loop(0, z.nt + z.nq)
    def _(u):
        for d in range(2):
            onward(u, d).wait_send()
        for x in range(3):
            own_to(u, x).wait_send()
            across(u, x).wait_send()
        for x in range(4):
            across_in(u, x).wait_recv()


def step(n, x, dy, weights, m, v):
    tokens, d = x.shape
    ff = weights[0].shape[2]
    z = types.SimpleNamespace(tokens=tokens, d=d, ff=ff, chips=n // 2, rows=d // n, fd=ff // n, tile=d // 2, block=512, ns_gu=3, ns_d=2)
    z.j = z.tile // LANES
    z.nt = ff // z.tile
    z.nq = z.fd // LANES
    z.nh = n // z.j
    assert z.chips == 4 and z.rows == LANES and z.nh == 2
    z.gap = z.nt
    units = z.nt + z.nq
    half = z.rows // 2
    q = z.nt
    z.early = 2
    z.s4b = ((2, 0), (4, 1), (6, q), (9, 2), (9, q + 2), (10, q + 3), (11, 6), (11, q + 1), (12, 7), (13, 3), (13, 5), (14, 4))
    z.s5b = ((3, 0), (5, 1), (13, q + 2), (15, q), (17, 4), (17, 5), (18, 3), (19, 7), (20, 2), (21, 6), (22, q + 1), (22, q + 3))
    z.s6b = ((4, 0), (8, 1), (18, q), (18, q + 2), (20, 3), (20, 4), (22, 2), (22, 6), (24, 5), (24, q + 3), (25, 7), (25, q + 1))
    held = (tokens // d, z.chips, 2, z.rows, d)

    def family(ns):
        dma, vm = pltpu.SemaphoreType.DMA, pltpu.VMEM
        return [
            vm((ns, z.chips, 2, z.rows, d), BF),
            vm((ns, z.chips, z.rows, d), BF),
            vm((ns, 2, z.rows, d), BF),
            vm((ns, 2, half, d), BF),
            vm((2, z.rows, d), BF),
            vm((2, half, d), BF),
            vm((z.rows, d), F32),
            vm((z.rows, d), F32),
            vm((z.rows, d), BF),
            vm((2, z.rows, d), BF),
            vm((2, z.rows, d), BF),
            dma((ns, 2)),
            dma((2,)),
            dma((ns, 2)),
            dma((2,)),
            dma((ns, 2)),
            pltpu.SemaphoreType.REGULAR((3,)),
            dma((9,)),
        ]

    dma, vm = pltpu.SemaphoreType.DMA, pltpu.VMEM
    return pl.pallas_call(
        functools.partial(step_kernel, z),
        in_specs=[pl.BlockSpec(memory_space=pl.ANY)] * 11,
        out_specs=[pl.BlockSpec(memory_space=pl.ANY)] * 8,
        out_shape=[
            jax.ShapeDtypeStruct((2 * units, z.rows, d), BF),
            jax.ShapeDtypeStruct((units, half, d), BF),
            jax.ShapeDtypeStruct((units, half, d), BF),
            jax.ShapeDtypeStruct((units, n, z.rows, d), BF),
            jax.ShapeDtypeStruct(held, BF),
            jax.ShapeDtypeStruct((tokens, d), BF),
            jax.ShapeDtypeStruct((z.nt - 2, tokens, z.tile), BF),
            jax.ShapeDtypeStruct((z.nt - 2, tokens, z.tile), BF),
        ],
        scratch_shapes=[
            vm((tokens, d), BF),
            vm((tokens, d), BF),
            vm((tokens, d), F32),
            vm((tokens, z.tile), BF),
            vm((2, tokens, z.tile), BF),
            vm((2, tokens, z.tile), BF),
            vm((2, d, z.tile), BF),
            vm((2, d, z.tile), BF),
            vm((2, z.tile, d), BF),
            *family(z.ns_gu),
            *family(z.ns_d),
            dma((2, 3)),
            dma((2,)),
            dma((8,)),
            dma((units, 3)),
            dma((units, 2)),
            dma((units, 2)),
            dma((units, 2)),
            dma((units, 3)),
            dma((units, 4)),
        ],
        compiler_params=pltpu.CompilerParams(collective_id=0, has_side_effects=True, vmem_limit_bytes=67043328),
        cost_estimate=pl.CostEstimate(flops=34 * tokens * d * ff, bytes_accessed=200 << 20, transcendentals=2 * tokens * ff),
        name="step",
    )(x.reshape(held), dy, *weights, *m, *v)[:4]


def place_kernel(z, layer, sources, count, *refs):
    srcs, (og, ou, od) = refs[:count], refs[count + 3 : count + 6]
    buf, gate, up, isem, osem = refs[count + 6 :]
    me = lax.axis_index("dp")
    c, k = me // 2, me % 2

    def source(x):
        at, other, part = sources[x]
        b = 2 * ((c + at) % z.chips) + (1 - k if other else k)
        return b, part, srcs[x].shape[1]

    def units(x):
        size = srcs[x].shape[0]
        return (z.nt if size == z.nq else 0), size, size != z.nq, size != z.nt

    def load(x):
        first, size, _, _ = units(x)
        return pltpu.make_async_copy(srcs[x], buf.at[x % 2, pl.ds(first, size), pl.ds(0, srcs[x].shape[1])], isem.at[x % 2])

    def stores(x):
        b, part, rows = source(x)
        r, s = pl.ds(part * rows, rows), pl.ds(0, rows)
        _, _, wide, deep = units(x)
        copies = (
            pltpu.make_async_copy(gate.at[x % 2, s], og.at[layer, b, r], osem.at[x % 2, 0]),
            pltpu.make_async_copy(up.at[x % 2, s], ou.at[layer, b, r], osem.at[x % 2, 1]),
            pltpu.make_async_copy(buf.at[x % 2, pl.ds(z.nt, z.nq), s], od.at[layer, b, :, r], osem.at[x % 2, 2]),
        )
        return copies[: 2 if wide else 0] + copies[2 : 3 if deep else 2]

    load(0).start()
    for x in range(count):
        load(x).wait()
        if x >= 1:
            for copy in stores(x - 1):
                copy.wait()
        if x + 1 < count:
            load(x + 1).start()
        rows = srcs[x].shape[1]
        for t in range(z.nt if units(x)[2] else 0):
            q, h = t // z.nh, t % z.nh
            for j in range(z.j):
                col = z.fd * (z.j * h + j) + LANES * q
                gate[x % 2, :rows, col : col + LANES] = buf[x % 2, t, :rows, LANES * j : LANES * (j + 1)]
                up[x % 2, :rows, col : col + LANES] = buf[x % 2, t, :rows, z.tile + LANES * j : z.tile + LANES * (j + 1)]
        for copy in stores(x):
            copy.start()
    for copy in stores(count - 1):
        copy.wait()


def place(z, layer, sources, arrays, outs):
    count = len(arrays)
    size = sum(a.size for a in arrays) * 4
    return pl.pallas_call(
        functools.partial(place_kernel, z, layer, sources, count),
        in_specs=[pl.BlockSpec(memory_space=pl.ANY)] * (count + 3),
        out_specs=[pl.BlockSpec(memory_space=pl.ANY)] * 3,
        out_shape=[jax.ShapeDtypeStruct(o.shape, o.dtype) for o in outs],
        input_output_aliases={count + i: i for i in range(3)},
        scratch_shapes=[
            pltpu.VMEM((2, z.nt + z.nq, z.rows, z.d), BF),
            pltpu.VMEM((2, z.rows, z.ff), BF),
            pltpu.VMEM((2, z.rows, z.ff), BF),
            pltpu.SemaphoreType.DMA((2,)),
            pltpu.SemaphoreType.DMA((2, 3)),
        ],
        compiler_params=pltpu.CompilerParams(vmem_limit_bytes=24 << 20),
        cost_estimate=pl.CostEstimate(flops=size * 100, bytes_accessed=size, transcendentals=0),
        name="place",
    )(*arrays, *outs)


def spread_kernel(z, src, og, ou, od):
    for t in range(z.nt):
        q, h = t // z.nh, t % z.nh
        for j in range(z.j):
            col = z.fd * (z.j * h + j) + LANES * q
            og[:, col : col + LANES] = src[t, :, LANES * j : LANES * (j + 1)]
            ou[:, col : col + LANES] = src[t, :, z.tile + LANES * j : z.tile + LANES * (j + 1)]
    od[...] = src[z.nt :]


def spread(z, layers, layer, agw):
    n = agw.shape[1]
    return pl.pallas_call(
        functools.partial(spread_kernel, z),
        grid=(n,),
        in_specs=[pl.BlockSpec((z.nt + z.nq, None, z.rows, z.d), lambda b: (0, b, 0, 0))],
        out_specs=[
            pl.BlockSpec((None, None, z.rows, z.ff), lambda b: (layer, b, 0, 0)),
            pl.BlockSpec((None, None, z.rows, z.ff), lambda b: (layer, b, 0, 0)),
            pl.BlockSpec((None, None, z.nq, z.rows, z.d), lambda b: (layer, b, 0, 0, 0)),
        ],
        out_shape=[
            jax.ShapeDtypeStruct((layers, n, z.rows, z.ff), BF),
            jax.ShapeDtypeStruct((layers, n, z.rows, z.ff), BF),
            jax.ShapeDtypeStruct((layers, n, z.nq, z.rows, z.d), BF),
        ],
        compiler_params=pltpu.CompilerParams(vmem_limit_bytes=24 << 20),
        cost_estimate=pl.CostEstimate(flops=agw.size * 400, bytes_accessed=agw.size * 4, transcendentals=0),
        name="spread",
    )(agw)


def moments(m, v, g):
    return 0.9 * m + 0.1 * g, 0.95 * v + 0.05 * g * g


def wide_moments_kernel(z, g, *refs):
    ins, outs = refs[:4], refs[4:]
    for t in range(z.nt):
        q, h = t // z.nh, t % z.nh
        for j in range(z.j):
            col = slice(z.fd * (z.j * h + j) + LANES * q, z.fd * (z.j * h + j) + LANES * (q + 1))
            for x in range(2):
                one = g[t, :, z.tile * x + LANES * j : z.tile * x + LANES * (j + 1)].astype(F32)
                outs[x][:, col], outs[x + 2][:, col] = moments(ins[x][:, col], ins[x + 2][:, col], one)


def wide_moments(z, g, mg, mu, vg, vu):
    layers, units = mg.shape[0], z.nt + z.nq
    rows = z.rows // 4
    block = pl.BlockSpec((None, rows, z.ff), lambda l, r: (l, r, 0))
    return pl.pallas_call(
        functools.partial(wide_moments_kernel, z),
        grid=(layers, 4),
        in_specs=[pl.BlockSpec((None, z.nt, rows, z.d), lambda l, r: (layers - 1 - l, 0, r, 0)), *[block] * 4],
        out_specs=[block] * 4,
        out_shape=[jax.ShapeDtypeStruct(mg.shape, F32)] * 4,
        compiler_params=pltpu.CompilerParams(vmem_limit_bytes=24 << 20),
        cost_estimate=pl.CostEstimate(flops=mg.size * 400, bytes_accessed=mg.size * 36, transcendentals=0),
        name="wide_moments",
    )(g.reshape(layers, units, z.rows, z.d), mg, mu, vg, vu)


def deep_moments_kernel(g, m, v, om, ov):
    om[...], ov[...] = moments(m[...], v[...], g[...].astype(F32))


def deep_moments(z, g, m, v):
    layers, units = m.shape[0], z.nt + z.nq
    block = pl.BlockSpec((None, z.rows, z.d), lambda l, q: (l, q, 0))
    return pl.pallas_call(
        deep_moments_kernel,
        grid=(layers, z.nq),
        in_specs=[pl.BlockSpec((None, None, z.rows, z.d), lambda l, q: (layers - 1 - l, z.nt + q, 0, 0)), block, block],
        out_specs=[block] * 2,
        out_shape=[jax.ShapeDtypeStruct(m.shape, F32)] * 2,
        compiler_params=pltpu.CompilerParams(vmem_limit_bytes=16 << 20),
        cost_estimate=pl.CostEstimate(flops=m.size * 200, bytes_accessed=m.size * 18, transcendentals=0),
        name="deep_moments",
    )(g.reshape(layers, units, z.rows, z.d), m, v)


def solution(mesh):
    n = mesh.shape["dp"]

    def device(x, dy, w_gate, w_up, w_down, *mv):
        m, v = mv[:3], mv[3:]
        x, dy = x[0], dy[0]
        layers, d, ff = w_gate.shape
        gown, wlo, whi, agw = step(n, x, dy, (w_gate, w_up, w_down), m, v)

        z = types.SimpleNamespace(d=d, ff=ff, chips=n // 2, rows=d // n, fd=ff // n, tile=d // 2)
        z.j, z.nt, z.nq = z.tile // LANES, ff // z.tile, z.fd // LANES
        z.nh = n // z.j
        after = lax.optimization_barrier

        def shift(a, by):
            return lax.ppermute(a, "dp", [(i, (i + 2 * by) % n) for i in range(n)])

        def swap(a):
            return lax.ppermute(a, "dp", [(i, i ^ 1) for i in range(n)])

        first = [shift(wlo, 1), shift(whi, -1)]
        second = [shift(whi, 1), shift(wlo, -1)]
        pair = [swap(wlo), swap(whi)]
        outs = spread(z, layers, 1, agw)
        mg, mu, vg, vu = wide_moments(z, gown, m[0], m[1], v[0], v[1])
        md, vd = deep_moments(z, gown, m[2], v[2])
        outs = place(z, 0, ((0, False, 0), (0, False, 1), (0, True, 0), (0, True, 1)), [wlo, whi, *pair], outs)
        first, second, outs, mg, md = after((first, second, outs, mg, md))
        far = [shift(first[0], 1), shift(first[1], -1)]
        pair_first = [swap(a) for a in first]
        pair_second = [swap(a) for a in second]
        outs = place(z, 0, ((-1, False, 0), (1, False, 1), (-1, True, 0), (1, True, 1)), [*first, *pair_first], outs)
        outs = place(z, 0, ((-1, False, 1), (1, False, 0), (-1, True, 1), (1, True, 0)), [*second, *pair_second], outs)
        far, outs = after((far, outs))
        pair_far = [swap(a) for a in far]
        outs = place(z, 0, ((2, False, 0), (2, False, 1)), far, outs)
        outs = place(z, 0, ((2, True, 0), (2, True, 1)), pair_far, outs)
        new = [o.reshape(w.shape) for o, w in zip(outs, (w_gate, w_up, w_down), strict=True)]
        return (*new, mg, mu, md, vg, vu, vd)

    sharded = P(None, "dp", None)
    return jax.shard_map(
        device,
        mesh=mesh,
        in_specs=(P(("rep", "dp")), P(("rep", "dp")), P(), P(), P(), *[sharded] * 6),
        out_specs=(*[P("rep")] * 3, *[P("rep", "dp", None)] * 6),
        check_vma=False,
    )
```

```python
import functools
import types

import jax
import jax.numpy as jnp
from jax import lax
from jax.experimental import pallas as pl
from jax.experimental.pallas import tpu as pltpu
from jax.sharding import PartitionSpec as P

MESH = pl.DeviceIdType.MESH
F32, BF = jnp.float32, jnp.bfloat16
LANES = 128


def dot(a, b, ca, cb):
    return lax.dot_general(a, b, (((ca,), (cb,)), ((), ())), preferred_element_type=F32)


def normed(h):
    wide = h.astype(F32)
    return (wide * lax.rsqrt(jnp.mean(wide * wide, -1, keepdims=True) + 1e-6)).astype(BF)


def new_weight(m, v, w, g):
    m = 0.9 * m + 0.1 * g
    v = 0.95 * v + 0.05 * g * g
    return w - 0.02 * (m * lax.rsqrt(v + 1e-8) + 0.1 * w)


def step_kernel(z, *refs):
    (xs, dy, wg, wu, wd, mg, mu, md, vg, vu, vd, gown, wlo, whi, agw, h1, a0, dgx, dux, a, dh, acc, act, dgs, dus, wbg, wbu, wbd), rest = refs[:28], refs[28:]
    families, (wsem, asem, xsem, adr, afr, ends) = rest[:36], rest[36:]
    names = ("u", "r0", "ra", "rb", "sa", "sb", "m", "v", "w", "gst", "wst", "q0", "q1s", "q1r", "q2s", "q2r", "cred", "qm")
    gu = types.SimpleNamespace(**dict(zip(names, families[:18], strict=True)), ns=z.ns_gu, total=2 * z.nt, first=z.nt, base=0)
    de = types.SimpleNamespace(**dict(zip(names, families[18:], strict=True)), ns=z.ns_d, total=2 * z.nq, first=z.nq, base=z.nt)
    gu.qo, gu.qg = gu.qm.at[3:7], gu.qm.at[7:9]
    de.qo, de.qg = de.qm.at[3:7], de.qm.at[7:9]

    me = lax.axis_index("dp")
    c, k, n = me // 2, me % 2, 2 * z.chips
    cp, cm, co = (c + 1) % z.chips, (c + z.chips - 1) % z.chips, (c + 2) % z.chips
    partner, plus, minus = 2 * c + 1 - k, 2 * cp + k, 2 * cm + k
    im, ip, io = 2 * cm + k, 2 * cp + k, 2 * co + k
    half = z.rows // 2
    lo, hi = pl.ds(0, half), pl.ds(half, half)
    to = (plus, minus)

    def rcopy(src, dst, ssem, rsem, dev):
        return pltpu.make_async_remote_copy(src_ref=src, dst_ref=dst, send_sem=ssem, recv_sem=rsem, device_id={"dp": dev}, device_id_type=MESH)

    barrier = pltpu.get_barrier_semaphore()
    for dev in (partner, plus, minus):
        pl.semaphore_signal(barrier, inc=1, device_id={"dp": dev}, device_id_type=MESH)

    def where(t):
        s = t % z.nt
        return 1 - t // z.nt, s // z.nh, s % z.nh

    def run_at(q, h, j):
        return pl.ds(pl.multiple_of(z.fd * (z.j * h + j) + LANES * q, LANES), LANES)

    def fetch(t, slot):
        l, q, h = where(t)
        for j in range(z.j):
            f, b = run_at(q, h, j), pl.ds(LANES * j, LANES)
            pltpu.make_async_copy(wg.at[l, :, f], wbg.at[slot, :, b], wsem.at[slot, 0]).start()
            pltpu.make_async_copy(wu.at[l, :, f], wbu.at[slot, :, b], wsem.at[slot, 1]).start()
            pltpu.make_async_copy(wd.at[l, f, :], wbd.at[slot, b, :], wsem.at[slot, 2]).start()

    def fetched(slot):
        pltpu.make_async_copy(wg.at[0, :, pl.ds(0, z.tile)], wbg.at[slot], wsem.at[slot, 0]).wait()
        pltpu.make_async_copy(wu.at[0, :, pl.ds(0, z.tile)], wbu.at[slot], wsem.at[slot, 1]).wait()
        pltpu.make_async_copy(wd.at[0, pl.ds(0, z.tile), :], wbd.at[slot], wsem.at[slot, 2]).wait()

    def part(f, slot, x, r):
        return f.u[slot, x, k, r, :].astype(F32) + f.r0[slot, x, r, :].astype(F32)

    def pair_copy(f, slot):
        return rcopy(f.u.at[slot, :, 1 - k], f.r0.at[slot], f.q0.at[slot, 0], f.q0.at[slot, 1], partner)

    def far_copy(f, slot, d):
        return rcopy(f.sa.at[d], f.ra.at[slot, d], f.q1s.at[d], f.q1r.at[slot, d], to[d])

    def near_copy(f, slot, d):
        return rcopy(f.sb.at[d], f.rb.at[slot, d], f.q2s.at[d], f.q2r.at[slot, d], to[d])

    def s0(f, v):
        slot = v % f.ns

        @pl.when(v >= f.ns)
        def _():
            pl.semaphore_wait(f.cred.at[0], 1)

        pair_copy(f, slot).start()

    def s1(f, v):
        slot = v % f.ns
        pair_copy(f, slot).wait_recv()

        @pl.when(v >= f.ns)
        def _():
            pl.semaphore_wait(f.cred.at[1], 1)
            pl.semaphore_wait(f.cred.at[2], 1)

        f.sa[0, lo, :] = part(f, slot, co, lo).astype(BF)
        f.sa[0, hi, :] = part(f, slot, cp, hi).astype(BF)
        f.sa[1, lo, :] = part(f, slot, cm, lo).astype(BF)
        f.sa[1, hi, :] = part(f, slot, co, hi).astype(BF)
        for d in range(2):
            far_copy(f, slot, d).start()

    def s2(f, v):
        slot = v % f.ns
        for d in range(2):
            far_copy(f, slot, d).wait_recv()
            far_copy(f, slot, d).wait_send()
        f.sb[0] = (part(f, slot, cp, lo) + f.ra[slot, 0, lo, :].astype(F32)).astype(BF)
        f.sb[1] = (part(f, slot, cm, hi) + f.ra[slot, 1, hi, :].astype(F32)).astype(BF)
        for d in range(2):
            near_copy(f, slot, d).start()
        f.load(v)

    def own_out(f, v, ws):
        return pltpu.make_async_copy(f.wst.at[ws], agw.at[f.base + v, me], f.qo.at[2 * ws])

    def last_out(f, v, ws, x):
        u = f.base + v - f.first
        return pltpu.make_async_copy(f.wst.at[ws, (lo, hi)[x]], (wlo, whi)[x].at[u], f.qo.at[2 * ws + x])

    def grad_out(f, v, ws):
        l = v // f.first
        return pltpu.make_async_copy(f.gst.at[ws], gown.at[l * (z.nt + z.nq) + f.base + v % f.first], f.qg.at[ws])

    def sent(f, v, ws):
        grad_out(f, v, ws).wait()

        @pl.when(v >= f.first)
        def _():
            for x in range(2):
                last_out(f, v, ws, x).wait()

    def s3(f, v):
        slot, ws = v % f.ns, v % 2

        @pl.when(v >= 2)
        def _():
            sent(f, v - 2, ws)

        for d in range(2):
            near_copy(f, slot, d).wait_recv()
            near_copy(f, slot, d).wait_send()
        pair_copy(f, slot).wait_send()
        f.loaded()
        for r, x in ((lo, 0), (hi, 1)):
            g = part(f, slot, c, r) + f.ra[slot, 1 - x, r, :].astype(F32) + f.rb[slot, x].astype(F32)
            g = g.astype(BF)
            f.gst[ws, r, :] = g
            f.wst[ws, r, :] = new_weight(f.m[r, :], f.v[r, :], f.w[r, :].astype(F32), g.astype(F32)).astype(BF)

        @pl.when(v + f.ns < f.total)
        def _():
            for x, dev in enumerate((partner, plus, minus)):
                pl.semaphore_signal(f.cred.at[x], inc=1, device_id={"dp": dev}, device_id_type=MESH)

        grad_out(f, v, ws).start()

        @pl.when(v < f.first)
        def _():
            own_out(f, v, ws).start()

        @pl.when(v >= f.first)
        def _():
            for x in range(2):
                last_out(f, v, ws, x).start()

    def own_to(u, x):
        return rcopy(agw.at[u, me], agw.at[u, me], ends.at[0], (adr.at[u, 0], adr.at[u, 1], ends.at[1])[x], (plus, minus, partner)[x])

    def near_in(u, d):
        return rcopy(agw.at[u, (im, ip)[d]], agw.at[u, (im, ip)[d]], ends.at[0], adr.at[u, d], to[d])

    def onward(u, d):
        x, r = ((im, lo), (ip, hi))[d]
        return rcopy(agw.at[u, x, r], agw.at[u, x, r], ends.at[0], afr.at[u, d], to[d])

    def far_in(u, d):
        r = (lo, hi)[d]
        return rcopy(agw.at[u, io, r], agw.at[u, io, r], ends.at[0], afr.at[u, d], to[d])

    def across(u, x):
        b = (im, ip, io)[x]
        return rcopy(agw.at[u, b], agw.at[u, b], ends.at[0], ends.at[1], partner)

    def gathered():
        rcopy(agw.at[:, : n - 1], agw.at[:, : n - 1], ends.at[0], ends.at[1], partner).wait_send()
        rcopy(agw.at[:, : n // 2], agw.at[:, : n // 2], ends.at[0], ends.at[1], partner).wait_recv()

    def held(f, v):
        @pl.when(v < f.first)
        def _():
            own_out(f, v, v % 2).wait()

    def s4(u):
        for x in range(3):
            own_to(u, x).start()

    def s5(u):
        for d in range(2):
            near_in(u, d).wait_recv()
            onward(u, d).start()
            across(u, d).start()

    def s6(u):
        for d in range(2):
            far_in(u, d).wait_recv()
        across(u, 2).start()

    def load_gu(v):
        l, q, h = where(v)
        for j in range(z.j):
            fr = run_at(q, h, j)
            for x, (m, vv, w) in enumerate(((mg, vg, wg), (mu, vu, wu))):
                b = pl.ds(z.tile * x + LANES * j, LANES)
                pltpu.make_async_copy(m.at[l, :, fr], gu.m.at[:, b], gu.qm.at[0]).start()
                pltpu.make_async_copy(vv.at[l, :, fr], gu.v.at[:, b], gu.qm.at[1]).start()
                pltpu.make_async_copy(w.at[l, pl.ds(me * z.rows, z.rows), fr], gu.w.at[:, b], gu.qm.at[2]).start()

    def loaded_gu():
        width = pl.ds(0, 2 * z.tile)
        pltpu.make_async_copy(mg.at[0, :, width], gu.m, gu.qm.at[0]).wait()
        pltpu.make_async_copy(vg.at[0, :, width], gu.v, gu.qm.at[1]).wait()
        pltpu.make_async_copy(wg.at[0, pl.ds(0, z.rows), width], gu.w, gu.qm.at[2]).wait()

    def d_copies(v):
        l, q = 1 - v // z.nq, v % z.nq
        r = pl.ds(pl.multiple_of(q * z.rows, z.rows), z.rows)
        return (
            pltpu.make_async_copy(md.at[l, r, :], de.m, de.qm.at[0]),
            pltpu.make_async_copy(vd.at[l, r, :], de.v, de.qm.at[1]),
            pltpu.make_async_copy(wd.at[l, pl.ds(pl.multiple_of(me * z.fd + q * z.rows, z.rows), z.rows), :], de.w, de.qm.at[2]),
        )

    def load_d(v):
        for copy in d_copies(v):
            copy.start()

    def loaded_d():
        for copy in d_copies(0):
            copy.wait()

    gu.load, gu.loaded, de.load, de.loaded = load_gu, loaded_gu, load_d, loaded_d

    def run(stage, f, made, least=0):
        if f is de:
            odd, made = made % 2 == 1, (made - 1) // 2
        gap = z.gap if f is gu else z.gap // 2
        v = jnp.where(made < f.first, made, made - gap)
        ok = jnp.logical_or(jnp.logical_and(made >= least, made < f.first), jnp.logical_and(made >= f.first + gap, made < f.total + gap))

        @pl.when(ok if f is gu else jnp.logical_and(ok, odd))
        def _():
            stage(f, v)

    def gather(stage, table, s):
        while table:
            once = dict(table)
            table = [pair for pair in table if once[pair[0]] != pair[1]]
            u, ok = 0, False
            for at, unit in once.items():
                u = jnp.where(s == at, unit, u)
                ok = jnp.logical_or(ok, s == at)

            @pl.when(ok)
            def _(u=u):
                stage(u)

    blocks = [pl.ds(r, z.block) for r in range(0, z.tokens, z.block)]

    def paired(body):
        @pl.loop(0, len(blocks) // 2)
        def _(i):
            for b in range(2):
                body(pl.ds(pl.multiple_of((2 * i + b) * z.block, z.block), z.block))

    per = z.chips * 2 * z.rows // z.block
    width = z.block // (2 * z.rows)

    def held_rows(b):
        return (b // per, pl.ds(b % per * width, width))

    def states(b):
        return gu.u[held_rows(b)].reshape(z.block, z.d)

    held_states = gu.u.at[: z.tokens * z.d // (z.chips * 2 * z.rows * z.d)]

    def x_in(b):
        return pltpu.make_async_copy(xs.at[held_rows(b)], gu.u.at[held_rows(b)], xsem.at[4 + b])

    for b in range(len(blocks)):
        x_in(b).start()
    fetch(z.nt, 0)
    pltpu.make_async_copy(dy, dh, asem.at[1]).start()

    def hidden(r, slot):
        g = dot(a[r, :], wbg[slot], 1, 0)
        u = dot(a[r, :], wbu[slot], 1, 0)
        act[r, :] = (g * (0.5 * jnp.tanh(0.5 * g) + 0.5) * u).astype(BF)

    x_in(0).wait()
    a[blocks[0], :] = normed(states(0))
    for b in range(1, len(blocks)):
        x_in(b).wait()
    fetched(0)
    fetch(z.nt + 1, 1)
    for b, r in enumerate(blocks):
        if b + 1 < len(blocks):
            a[blocks[b + 1], :] = normed(states(b + 1))
        hidden(r, 0)
    pltpu.make_async_copy(a, a0, xsem.at[1]).start()
    for r in blocks:
        acc[r, :] = dot(act[r, :], wbd[0], 1, 0)

    @pl.loop(1, z.nt)
    def _(t):
        slot = t % 2
        fetched(slot)
        fetch(jnp.where(t + 1 < z.nt, t + 1 + z.nt, 0), 1 - slot)
        for r in blocks:
            hidden(r, slot)

        @pl.when(t < z.nt - 1)
        def _():
            for r in blocks:
                acc[r, :] += dot(act[r, :], wbd[slot], 1, 0)

    pltpu.make_async_copy(a, a0, xsem.at[1]).wait()
    for b, r in enumerate(blocks):
        y = (acc[r, :] + dot(act[r, :], wbd[(z.nt - 1) % 2], 1, 0)).astype(BF)
        h = (states(b).astype(F32) + y.astype(F32)).astype(BF)
        gu.u[held_rows(b)] = h.reshape(width, 2, z.rows, z.d)
        a[r, :] = normed(h)
    acc[...] = jnp.zeros_like(acc)
    pltpu.make_async_copy(held_states, h1, xsem.at[0]).start()
    pltpu.make_async_copy(dy, dh, asem.at[1]).wait()
    pl.semaphore_wait(barrier, 3)

    end = 2 * z.nt + z.gap

    def spill(t, slot):
        return (
            pltpu.make_async_copy(dgs.at[slot], dgx.at[t], xsem.at[2]),
            pltpu.make_async_copy(dus.at[slot], dux.at[t], xsem.at[3]),
        )

    def unspill(t, slot):
        return (
            pltpu.make_async_copy(dgx.at[t], dgs.at[slot], xsem.at[4 + slot]),
            pltpu.make_async_copy(dux.at[t], dus.at[slot], xsem.at[6 + slot]),
        )

    def add_da(t, slot):
        @pl.when(t < z.nt - 2)
        def _():
            for copy in unspill(t, slot):
                copy.wait()
            fetched(slot)

        @paired
        def _(r):
            acc[r, :] += dot(dgs[slot, r, :], wbg[slot], 1, 1) + dot(dus[slot, r, :], wbu[slot], 1, 1)

        @pl.when(t >= 2)
        def _():
            fetch(t - 2, slot)
            for copy in unspill(t - 2, slot):
                copy.start()

    staged = (("g3", s3, gu), ("g2", s2, gu), ("d1", s1, de), ("d3", s3, de), ("d2", s2, de))

    def stages(place, s):
        for name, stage, f in staged:
            lag, at = z.lags[name]
            if at == place:
                run(stage, f, s - lag, z.early if name[0] == "g" else 0)

    @pl.loop(0, end + 2)
    def _(s):
        second = s >= z.nt + z.gap
        t = jnp.where(second, s - z.gap, s)
        slot = t % 2
        working = jnp.logical_and(s < end, jnp.logical_or(second, s < z.nt))
        adding = jnp.logical_and(s >= z.nt, jnp.logical_not(second))

        @pl.when(working)
        def _():
            fetched(slot)

            @pl.when(t % z.nt < z.nt - 1)
            def _():
                fetch(t + 1, 1 - slot)

        stages(0, s)

        @pl.when(working)
        def _():
            @pl.when(t == z.nt)
            def _():
                pltpu.make_async_copy(a0, a, asem.at[0]).wait()

            @paired
            def _(r):
                da = dot(dh[r, :], wbd[slot], 1, 1).astype(BF).astype(F32)
                g = dot(a[r, :], wbg[slot], 1, 0)
                u = dot(a[r, :], wbu[slot], 1, 0)
                sig = 0.5 * jnp.tanh(0.5 * g) + 0.5
                gs = g * sig
                act[r, :] = (gs * u).astype(BF)
                dgs[slot, r, :] = (da * (u * (sig + gs * (1.0 - sig)))).astype(BF)
                dus[slot, r, :] = (da * gs).astype(BF)

            @pl.when(t < z.nt - 2)
            def _():
                for copy in spill(t, slot):
                    copy.start()

        @pl.when(s == z.early)
        def _():
            s2(gu, 0)

        @pl.when(s == z.early + 1)
        def _():
            held(gu, 0)

        run(held, de, s - 3)
        gather(s4, z.s4b, s)
        gather(s5, z.s5b, s)
        gather(s6, z.s6b, s)

        @pl.when(s == end + 1)
        def _():
            gathered()

        stages(1, s)

        @pl.when(s == 0)
        def _():
            pltpu.make_async_copy(held_states, h1, xsem.at[0]).wait()

        @pl.when(adding)
        def _():
            tile = 2 * z.nt - 1 - s
            add_da(tile, tile % 2)

        @pl.when(working)
        def _():
            us = t % gu.ns
            shape = (z.chips, 2, z.rows, z.tile)
            gu.u[us, :, :, :, : z.tile] = dot(a[...], dgs[slot], 0, 0).astype(BF).reshape(shape)
            gu.u[us, :, :, :, z.tile :] = dot(a[...], dus[slot], 0, 0).astype(BF).reshape(shape)

            @pl.when(t == z.nt - 1)
            def _():
                for b in range(z.tokens // z.rows):
                    at = h1.at[b // (2 * z.chips), b // 2 % z.chips, b % 2]
                    pltpu.make_async_copy(at, a.at[pl.ds(z.rows * b, z.rows)], asem.at[0]).start()

            @pl.when(t < z.nt - 2)
            def _():
                for copy in spill(t, slot):
                    copy.wait()

        run(s0, gu, s)
        run(held, gu, s - 3, z.early)
        stages(2, s)

        @pl.when(working)
        def _():
            gd = dot(act[...], dh[...], 0, 0).astype(BF).reshape(z.j // 2, 2, z.rows, z.d)
            de.u[(t // 2) % de.ns, pl.ds((t % 2) * (z.j // 2), z.j // 2)] = gd

        run(s1, gu, s)
        run(s0, de, s)
        stages(3, s)

        @pl.when(s == z.early)
        def _():
            s3(gu, 0)

        @pl.when(s == z.nt + z.gap - 1)
        def _():
            fetch(z.nt, 0)
            pltpu.make_async_copy(a0, a, asem.at[0]).wait()

            @pl.loop(0, z.tokens // z.block)
            def _(i):
                r = pl.ds(pl.multiple_of(i * z.block, z.block), z.block)
                h = a[r, :].astype(F32)
                da = acc[r, :].astype(BF).astype(F32)
                scale = lax.rsqrt(jnp.mean(h * h, -1, keepdims=True) + 1e-6)
                along = jnp.mean(da * h, -1, keepdims=True)
                by_h = (scale * da - h * (scale * scale * scale * along)).astype(BF)
                dh[r, :] = (dh[r, :].astype(F32) + by_h.astype(F32)).astype(BF)

            pltpu.make_async_copy(a0, a, asem.at[0]).start()

    for f in (gu, de):
        for v in (f.total - 2, f.total - 1):
            sent(f, v, v % 2)


def step(n, x, dy, weights, m, v):
    tokens, d = x.shape
    ff = weights[0].shape[2]
    z = types.SimpleNamespace(tokens=tokens, d=d, ff=ff, chips=n // 2, rows=d // n, fd=ff // n, tile=d // 2, block=512, ns_gu=3, ns_d=2)
    z.j = z.tile // LANES
    z.nt = ff // z.tile
    z.nq = z.fd // LANES
    z.nh = n // z.j
    assert z.chips == 4 and z.rows == LANES and z.nh == 2
    z.gap = z.nt
    units = z.nt + z.nq
    half = z.rows // 2
    q = z.nt
    z.early = 1
    z.lags = {"g2": (1, 2), "g3": (2, 2), "d1": (1, 1), "d2": (2, 0), "d3": (2, 3)}
    z.s4b = ((3, 0), (5, 1), (7, q), (9, 3), (10, 4), (11, q + 1), (11, q + 3), (13, 5), (13, q + 2), (16, 6), (19, 2), (21, 7))
    z.s5b = ((10, 0), (13, 4), (14, 1), (15, q + 1), (15, q + 3), (16, q), (16, q + 2), (17, 5), (17, 6), (19, 3), (23, 2), (23, 7))
    z.s6b = ((17, 0), (17, q + 2), (18, 6), (19, 4), (19, q + 3), (20, 3), (20, q + 1), (23, 5), (24, 2), (24, q), (25, 1), (25, 7))
    held = (tokens // d, z.chips, 2, z.rows, d)

    def family(ns):
        dma, vm = pltpu.SemaphoreType.DMA, pltpu.VMEM
        return [
            vm((ns, z.chips, 2, z.rows, d), BF),
            vm((ns, z.chips, z.rows, d), BF),
            vm((ns, 2, z.rows, d), BF),
            vm((ns, 2, half, d), BF),
            vm((2, z.rows, d), BF),
            vm((2, half, d), BF),
            vm((z.rows, d), F32),
            vm((z.rows, d), F32),
            vm((z.rows, d), BF),
            vm((2, z.rows, d), BF),
            vm((2, z.rows, d), BF),
            dma((ns, 2)),
            dma((2,)),
            dma((ns, 2)),
            dma((2,)),
            dma((ns, 2)),
            pltpu.SemaphoreType.REGULAR((3,)),
            dma((9,)),
        ]

    dma, vm = pltpu.SemaphoreType.DMA, pltpu.VMEM
    return pl.pallas_call(
        functools.partial(step_kernel, z),
        in_specs=[pl.BlockSpec(memory_space=pl.ANY)] * 11,
        out_specs=[pl.BlockSpec(memory_space=pl.ANY)] * 8,
        out_shape=[
            jax.ShapeDtypeStruct((2 * units, z.rows, d), BF),
            jax.ShapeDtypeStruct((units, half, d), BF),
            jax.ShapeDtypeStruct((units, half, d), BF),
            jax.ShapeDtypeStruct((units, n, z.rows, d), BF),
            jax.ShapeDtypeStruct(held, BF),
            jax.ShapeDtypeStruct((tokens, d), BF),
            jax.ShapeDtypeStruct((z.nt - 2, tokens, z.tile), BF),
            jax.ShapeDtypeStruct((z.nt - 2, tokens, z.tile), BF),
        ],
        scratch_shapes=[
            vm((tokens, d), BF),
            vm((tokens, d), BF),
            vm((tokens, d), F32),
            vm((tokens, z.tile), BF),
            vm((2, tokens, z.tile), BF),
            vm((2, tokens, z.tile), BF),
            vm((2, d, z.tile), BF),
            vm((2, d, z.tile), BF),
            vm((2, z.tile, d), BF),
            *family(z.ns_gu),
            *family(z.ns_d),
            dma((2, 3)),
            dma((2,)),
            dma((8,)),
            dma((units, 2)),
            dma((units, 2)),
            dma((2,)),
        ],
        compiler_params=pltpu.CompilerParams(collective_id=0, has_side_effects=True, vmem_limit_bytes=67043328),
        cost_estimate=pl.CostEstimate(flops=34 * tokens * d * ff, bytes_accessed=200 << 20, transcendentals=2 * tokens * ff),
        name="step",
    )(x.reshape(held), dy, *weights, *m, *v)[:4]


def place_kernel(z, layer, sources, count, *refs):
    srcs, (og, ou, od) = refs[:count], refs[count + 3 : count + 6]
    buf, gate, up, isem, osem = refs[count + 6 :]
    me = lax.axis_index("dp")
    c, k = me // 2, me % 2

    def source(x):
        at, other, part = sources[x]
        b = 2 * ((c + at) % z.chips) + (1 - k if other else k)
        return b, part, srcs[x].shape[1]

    def units(x):
        size = srcs[x].shape[0]
        return (z.nt if size == z.nq else 0), size, size != z.nq, size != z.nt

    def load(x):
        first, size, _, _ = units(x)
        return pltpu.make_async_copy(srcs[x], buf.at[x % 2, pl.ds(first, size), pl.ds(0, srcs[x].shape[1])], isem.at[x % 2])

    def stores(x):
        b, part, rows = source(x)
        r, s = pl.ds(part * rows, rows), pl.ds(0, rows)
        _, _, wide, deep = units(x)
        copies = (
            pltpu.make_async_copy(gate.at[x % 2, s], og.at[layer, b, r], osem.at[x % 2, 0]),
            pltpu.make_async_copy(up.at[x % 2, s], ou.at[layer, b, r], osem.at[x % 2, 1]),
            pltpu.make_async_copy(buf.at[x % 2, pl.ds(z.nt, z.nq), s], od.at[layer, b, :, r], osem.at[x % 2, 2]),
        )
        return copies[: 2 if wide else 0] + copies[2 : 3 if deep else 2]

    load(0).start()
    for x in range(count):
        load(x).wait()
        if x >= 1:
            for copy in stores(x - 1):
                copy.wait()
        if x + 1 < count:
            load(x + 1).start()
        rows = srcs[x].shape[1]
        if units(x)[2]:

            @pl.loop(0, z.nt)
            def _(t, x=x, rows=rows):
                q, h = t // z.nh, t % z.nh
                for j in range(z.j):
                    to = pl.ds(pl.multiple_of(z.fd * (z.j * h + j) + LANES * q, LANES), LANES)
                    gate[x % 2, :rows, to] = buf[x % 2, t, :rows, LANES * j : LANES * (j + 1)]
                    up[x % 2, :rows, to] = buf[x % 2, t, :rows, z.tile + LANES * j : z.tile + LANES * (j + 1)]

        for copy in stores(x):
            copy.start()
    for copy in stores(count - 1):
        copy.wait()


def place(z, layer, sources, arrays, outs):
    count = len(arrays)
    size = sum(a.size for a in arrays) * 4
    return pl.pallas_call(
        functools.partial(place_kernel, z, layer, sources, count),
        in_specs=[pl.BlockSpec(memory_space=pl.ANY)] * (count + 3),
        out_specs=[pl.BlockSpec(memory_space=pl.ANY)] * 3,
        out_shape=[jax.ShapeDtypeStruct(o.shape, o.dtype) for o in outs],
        input_output_aliases={count + i: i for i in range(3)},
        scratch_shapes=[
            pltpu.VMEM((2, z.nt + z.nq, z.rows, z.d), BF),
            pltpu.VMEM((2, z.rows, z.ff), BF),
            pltpu.VMEM((2, z.rows, z.ff), BF),
            pltpu.SemaphoreType.DMA((2,)),
            pltpu.SemaphoreType.DMA((2, 3)),
        ],
        compiler_params=pltpu.CompilerParams(vmem_limit_bytes=24 << 20),
        cost_estimate=pl.CostEstimate(flops=size * 100, bytes_accessed=size, transcendentals=0),
        name="place",
    )(*arrays, *outs)


def spread_kernel(z, src, og, ou, od):
    for t in range(z.nt):
        q, h = t // z.nh, t % z.nh
        for j in range(z.j):
            col = z.fd * (z.j * h + j) + LANES * q
            og[:, col : col + LANES] = src[t, :, LANES * j : LANES * (j + 1)]
            ou[:, col : col + LANES] = src[t, :, z.tile + LANES * j : z.tile + LANES * (j + 1)]
    od[...] = src[z.nt :]


def spread(z, layers, layer, agw):
    n = agw.shape[1]
    return pl.pallas_call(
        functools.partial(spread_kernel, z),
        grid=(n,),
        in_specs=[pl.BlockSpec((z.nt + z.nq, None, z.rows, z.d), lambda b: (0, b, 0, 0))],
        out_specs=[
            pl.BlockSpec((None, None, z.rows, z.ff), lambda b: (layer, b, 0, 0)),
            pl.BlockSpec((None, None, z.rows, z.ff), lambda b: (layer, b, 0, 0)),
            pl.BlockSpec((None, None, z.nq, z.rows, z.d), lambda b: (layer, b, 0, 0, 0)),
        ],
        out_shape=[
            jax.ShapeDtypeStruct((layers, n, z.rows, z.ff), BF),
            jax.ShapeDtypeStruct((layers, n, z.rows, z.ff), BF),
            jax.ShapeDtypeStruct((layers, n, z.nq, z.rows, z.d), BF),
        ],
        compiler_params=pltpu.CompilerParams(vmem_limit_bytes=24 << 20),
        cost_estimate=pl.CostEstimate(flops=agw.size * 400, bytes_accessed=agw.size * 4, transcendentals=0),
        name="spread",
    )(agw)


def moments(m, v, g):
    return 0.9 * m + 0.1 * g, 0.95 * v + 0.05 * g * g


def wide_moments_kernel(z, g, *refs):
    ins, outs = refs[:4], refs[4:]
    for t in range(z.nt):
        q, h = t // z.nh, t % z.nh
        for j in range(z.j):
            col = slice(z.fd * (z.j * h + j) + LANES * q, z.fd * (z.j * h + j) + LANES * (q + 1))
            for x in range(2):
                one = g[t, :, z.tile * x + LANES * j : z.tile * x + LANES * (j + 1)].astype(F32)
                outs[x][:, col], outs[x + 2][:, col] = moments(ins[x][:, col], ins[x + 2][:, col], one)


def wide_moments(z, g, mg, mu, vg, vu):
    layers, units = mg.shape[0], z.nt + z.nq
    rows = z.rows // 4
    block = pl.BlockSpec((None, rows, z.ff), lambda l, r: (l, r, 0))
    return pl.pallas_call(
        functools.partial(wide_moments_kernel, z),
        grid=(layers, 4),
        in_specs=[pl.BlockSpec((None, z.nt, rows, z.d), lambda l, r: (layers - 1 - l, 0, r, 0)), *[block] * 4],
        out_specs=[block] * 4,
        out_shape=[jax.ShapeDtypeStruct(mg.shape, F32)] * 4,
        compiler_params=pltpu.CompilerParams(vmem_limit_bytes=24 << 20),
        cost_estimate=pl.CostEstimate(flops=mg.size * 400, bytes_accessed=mg.size * 36, transcendentals=0),
        name="wide_moments",
    )(g.reshape(layers, units, z.rows, z.d), mg, mu, vg, vu)


def deep_moments_kernel(g, m, v, om, ov):
    om[...], ov[...] = moments(m[...], v[...], g[...].astype(F32))


def deep_moments(z, g, m, v):
    layers, units = m.shape[0], z.nt + z.nq
    block = pl.BlockSpec((None, z.rows, z.d), lambda l, q: (l, q, 0))
    return pl.pallas_call(
        deep_moments_kernel,
        grid=(layers, z.nq),
        in_specs=[pl.BlockSpec((None, None, z.rows, z.d), lambda l, q: (layers - 1 - l, z.nt + q, 0, 0)), block, block],
        out_specs=[block] * 2,
        out_shape=[jax.ShapeDtypeStruct(m.shape, F32)] * 2,
        compiler_params=pltpu.CompilerParams(vmem_limit_bytes=16 << 20),
        cost_estimate=pl.CostEstimate(flops=m.size * 200, bytes_accessed=m.size * 18, transcendentals=0),
        name="deep_moments",
    )(g.reshape(layers, units, z.rows, z.d), m, v)


def solution(mesh):
    n = mesh.shape["dp"]

    def device(x, dy, w_gate, w_up, w_down, *mv):
        m, v = mv[:3], mv[3:]
        x, dy = x[0], dy[0]
        layers, d, ff = w_gate.shape
        gown, wlo, whi, agw = step(n, x, dy, (w_gate, w_up, w_down), m, v)

        z = types.SimpleNamespace(d=d, ff=ff, chips=n // 2, rows=d // n, fd=ff // n, tile=d // 2)
        z.j, z.nt, z.nq = z.tile // LANES, ff // z.tile, z.fd // LANES
        z.nh = n // z.j
        after = lax.optimization_barrier

        def shift(a, by):
            return lax.ppermute(a, "dp", [(i, (i + 2 * by) % n) for i in range(n)])

        def swap(a):
            return lax.ppermute(a, "dp", [(i, i ^ 1) for i in range(n)])

        first = [shift(wlo, 1), shift(whi, -1)]
        pair = [swap(wlo), swap(whi)]
        second = [shift(whi, 1), shift(wlo, -1)]
        md, vd = deep_moments(z, gown, m[2], v[2])
        mg, mu, vg, vu = wide_moments(z, gown, m[0], m[1], v[0], v[1])
        outs = spread(z, layers, 1, agw)
        outs = place(z, 0, ((0, False, 0), (0, False, 1), (0, True, 0), (0, True, 1)), [wlo, whi, *pair], outs)
        first, outs, mg, md = after((first, outs, mg, md))
        far_wide = [shift(first[0][: z.nt], 1), shift(first[1][: z.nt], -1)]
        far_deep = [shift(first[0][z.nt :], 1), shift(first[1][z.nt :], -1)]
        pair_first = [swap(a) for a in first]
        outs = place(z, 0, ((-1, False, 0), (1, False, 1), (-1, True, 0), (1, True, 1)), [*first, *pair_first], outs)
        second, outs = after((second, outs))
        pair_second = [swap(a) for a in second]
        outs = place(z, 0, ((-1, False, 1), (1, False, 0), (-1, True, 1), (1, True, 0)), [*second, *pair_second], outs)
        for far in (far_wide, far_deep):
            far, outs = after((far, outs))
            pair_far = [swap(a) for a in far]
            outs = place(z, 0, ((2, False, 0), (2, False, 1)), far, outs)
            outs = place(z, 0, ((2, True, 0), (2, True, 1)), pair_far, outs)
        new = [o.reshape(w.shape) for o, w in zip(outs, (w_gate, w_up, w_down), strict=True)]
        return (*new, mg, mu, md, vg, vu, vd)

    sharded = P(None, "dp", None)
    return jax.shard_map(
        device,
        mesh=mesh,
        in_specs=(P(("rep", "dp")), P(("rep", "dp")), P(), P(), P(), *[sharded] * 6),
        out_specs=(*[P("rep")] * 3, *[P("rep", "dp", None)] * 6),
        check_vma=False,
    )
```
